512 devices in a mesh: dp: 128 (over x, z, core), mp: 4 (over y).
Axes of the slice: x: 4, y: 4, z: 16, core: 2. Of those that a mesh axis runs over, the one named last changes fastest.
Arguments:
- gating_logits: bfloat16 [128, 3, 64, 7168], P('dp', None, None, 'mp'), may hold values from -6 to 6
- lifted_hidden_values: bfloat16 [128, 3, 64, 7168], P('dp', None, None, 'mp'), may hold values from -6 to 6
- loss_output_grad: bfloat16 [128, 3, 64, 2048], P('dp', None, None, 'mp'), may hold values from -1792 to 1792
- arrival_flags: int32 [128], P('dp'), may hold values from 0 to 1, as said below
- block_owner_map: int32 [128, 3], P('dp'), may hold values from 0 to 127, as said below
- decoder_multipliers: int32 [128, 3], P('dp'), may hold values from 1 to 4
- block_piece_number: int32 [128], replicated, may hold values from 1 to 2, as said below
Outputs:
- down_grad: float32 [2048, 7168], P('dp', 'mp')
The draws below stay inside these ranges and needn't reach their ends.
Inputs may be any that keep to these rules, and one draw needn't show every extreme that they name: `arrival_flags`: at least one replica survives. `block_owner_map`: row i lists the partitions (i + r + k) mod 128 for k < 3, with one r for all rows. `block_piece_number`: some partition has exactly 2 live tiles.
All inputs are finite; a program needn't handle non-finite values.
Results may differ from the reference program's by a relative error of at most 0.0042.
Values may be sent and summed in bfloat16 or wider, within the bound.
A program may use at most 128 MiB of HBM per device.

```python
import jax
import jax.numpy as jnp
from jax import lax

D = 2048
SLOTS = 3
TILE = 32
TILES = 2
TOK = 64
FF = 7168
N_DP = 128


def draw_arrival_flags(key, part):
    coin_flips = jax.random.randint(jax.random.fold_in(key, 11), (N_DP,), 0, 4)
    forced = jax.random.randint(jax.random.fold_in(key, 12), (), 0, N_DP)
    alive = jnp.where(coin_flips > 0, 1, 0)
    return jnp.where(jnp.arange(N_DP) == forced, 1, alive).astype(jnp.int32)


def draw_block_owner_map(key, part):
    rotation = jax.random.randint(jax.random.fold_in(key, 21), (), 0, N_DP)
    rows_idx = jnp.arange(N_DP, dtype=jnp.int32)[:, None]
    slot_idx = jnp.arange(SLOTS, dtype=jnp.int32)[None, :]
    return ((rows_idx + rotation + slot_idx) % N_DP).astype(jnp.int32)


def draw_block_piece_number(key, part):
    part_ids = jnp.arange(N_DP, dtype=jnp.int32)
    baseline = 1 + part_ids * (TILES - 1) // max(N_DP - 1, 1)
    jitter = jax.random.randint(jax.random.fold_in(key, 31), (N_DP,), 0, 2)
    return jnp.minimum(baseline + jitter, TILES).astype(jnp.int32)


def plant(array, own_key, low, high):
    shape = array.shape
    spot = [jax.random.randint(jax.random.fold_in(own_key, axis), (), 0, shape[axis]) for axis in range(len(shape))]
    array = array.at[tuple(spot)].set(low)
    longest = shape.index(max(shape))
    spot[longest] = (spot[longest] + 1) % shape[longest]
    return array.at[tuple(spot)].set(high)


def strengthened(entries, key, source, target, blocks, factor):
    owner, partner = [(jnp.arange(entries.shape[dim]) // (entries.shape[dim] // blocks)).reshape([-1 if axis == dim else 1 for axis in range(entries.ndim)]) for dim in (source, target)]
    chosen = jax.random.permutation(key, blocks)[partner]
    strong = (owner == chosen) | (owner == (partner + blocks // 2) % blocks)
    return jnp.where(strong, factor * entries, entries)


def shard_levels(own_key, extent, cuts, smallest, top_value):
    gain, own = 1.0, jax.random.fold_in(own_key, 6)
    for axis_at, blocks in cuts:
        steps = jnp.exp(jax.random.uniform(jax.random.fold_in(own, axis_at), (blocks,), jnp.float32, smallest / len(cuts), top_value / len(cuts)))
        gain = gain * jnp.repeat(steps, extent[axis_at] // blocks).reshape([-1 if axis == axis_at else 1 for axis in range(len(extent))])
    return gain


def normal_values(rng, dims, deviation, reach, cuts=(), held_as=jnp.bfloat16):
    result = deviation * jax.random.normal(rng, dims, jnp.float32)
    if cuts:
        result = result * shard_levels(rng, dims, cuts, -0.22, 0.18)
    return jnp.clip(result, -reach, reach).astype(held_as)


def noise_with(own_key, shape, scale, limit, cuts, heavy, held_as=jnp.bfloat16):
    result = scale * jax.random.normal(own_key, shape, jnp.float32)
    if cuts:
        result = result * shard_levels(own_key, shape, cuts, -0.22, 0.18)
    return jnp.clip(strengthened(result, jax.random.fold_in(own_key, 3), *heavy), -limit, limit).astype(held_as)


def setup_inputs(seed: int = 0) -> dict:
    key_of = jax.random.split(jax.random.key(seed), 8)
    return {
        "gating_logits": normal_values(key_of[0], (N_DP, SLOTS, TOK, FF), 1.0, 6.0, ((0, 128), (3, 4))),
        "lifted_hidden_values": normal_values(key_of[1], (N_DP, SLOTS, TOK, FF), 1.0, 6.0, ((0, 128), (3, 4))),
        "loss_output_grad": noise_with(key_of[2], (N_DP, SLOTS, TOK, D), ((N_DP * SLOTS * TOK) ** 0.5 / 2), 1792.0, ((0, 128), (3, 4)), (0, 3, 128, 5.5)),
        "arrival_flags": draw_arrival_flags(jax.random.fold_in(key_of[7], 71), 0),
        "block_owner_map": draw_block_owner_map(jax.random.fold_in(key_of[7], 71), 0),
        "decoder_multipliers": plant(jax.random.randint(key_of[5], (N_DP, SLOTS), 1, 5), jax.random.fold_in(key_of[5], 1), 1, 4).astype(jnp.int32),
        "block_piece_number": draw_block_piece_number(jax.random.fold_in(key_of[7], 71), 0),
    }


def reference(gating_logits, lifted_hidden_values, loss_output_grad, arrival_flags, block_owner_map, decoder_multipliers, block_piece_number):
    part_ids = jnp.arange(N_DP, dtype=jnp.int32)
    slot_tiles = jnp.sum(jnp.where(block_owner_map[:, :, None] == part_ids[None, None, :], block_piece_number[None, None, :], 0), axis=2)
    live_rows = slot_tiles * TILE
    live_mask = jnp.arange(TOK, dtype=jnp.int32)[None, None, :] < live_rows[:, :, None]
    down_kernel_array = arrival_flags[:, None].astype(jnp.float32) * decoder_multipliers.astype(jnp.float32)
    total_tokens = jnp.sum(down_kernel_array * live_rows.astype(jnp.float32))

    def accumulate(running_total, current_inputs):
        gate_now, current_up_projection, cot_now, weight_now, live_now = current_inputs
        hidden = (jax.nn.silu(gate_now.astype(jnp.float32)) * current_up_projection.astype(jnp.float32) * live_now[:, :, None].astype(jnp.float32)).astype(jnp.bfloat16)
        scaled = hidden.astype(jnp.float32) * weight_now[:, None, None]
        contrib = jnp.einsum("ktd,ktf->df", cot_now.astype(jnp.float32), scaled, precision=lax.Precision.HIGHEST)
        return running_total + contrib, None

    start_sum = jnp.zeros((D, FF), jnp.float32)
    coded, _ = lax.scan(accumulate, start_sum, (gating_logits, lifted_hidden_values, loss_output_grad, down_kernel_array, live_mask))
    return coded / total_tokens
```

```python
import functools

import jax
import jax.numpy as jnp
from jax import lax
from jax.experimental import pallas as pl
from jax.experimental.pallas import tpu as pltpu
from jax.sharding import PartitionSpec as P

MESH = pl.DeviceIdType.MESH
TILE = 32
NX = 4
NY = 4
NC = 2
PAD = 16
WIDTHS = (384, 256, 256)
STAGGER = 3
CHAINS = ((1, (7, 6, 5, 4, 3, 2, 1, 0)), (-1, (8, 7, 6, 5, 4, 3, 2, 1, 0)))
SEMS = 192


def kernel(
    nz, slots, tok,
    gate_hbm, lift_hbm, cot_hbm, arrival, owner, mult, pieces,
    out,
    gate, lift, cot, in_sem,
    Y, TU, TD, C, CT, H, HS, PR, ZS, ZR, CS, CR, R, FR, cnt_z,
    ssem, rsem,
):
    T = slots * tok
    TP = T + PAD
    nq = len(WIDTHS)
    half = sum(WIDTHS)
    offs = [sum(WIDTHS[:q]) for q in range(nq)]
    LO = (T // 2) // 16 * 16

    dp = lax.axis_index("dp")
    y = lax.axis_index("mp")
    x = dp // (NC * nz)
    z = (dp // NC) % nz
    c = dp % NC

    def dev(dx=0, dy=0, dz=0, flip=False):
        xx = (x + dx + NX) % NX
        yy = (y + dy + NY) % NY
        zz = (z + dz + nz) % nz
        cc = 1 - c if flip else c
        return (xx * (NC * nz) + zz * NC + cc, yy)

    ids = iter(range(SEMS))
    every = []

    def send(src, dst, to):
        i = next(ids)
        d = pltpu.make_async_remote_copy(
            src_ref=src, dst_ref=dst, send_sem=ssem.at[i], recv_sem=rsem.at[i],
            device_id=to, device_id_type=MESH,
        )
        d.start()
        every.append(d)
        return d

    loads = [
        pltpu.make_async_copy(cot_hbm, cot, in_sem.at[0]),
        pltpu.make_async_copy(gate_hbm, gate, in_sem.at[1]),
        pltpu.make_async_copy(lift_hbm, lift, in_sem.at[2]),
    ]
    for d in loads:
        d.start()

    hops = sorted({a - b for _, dist in CHAINS for a, b in zip(dist, dist[1:])})
    near = [dev(flip=True), dev(dx=1), dev(dx=-1), dev(dy=1), dev(dy=-1)]
    for h in hops:
        near += [dev(dz=h), dev(dz=-h)]
    barrier = pltpu.get_barrier_semaphore()
    for n in near:
        pl.semaphore_signal(barrier, inc=1, device_id=n, device_id_type=MESH)
    pl.semaphore_wait(barrier, len(near))

    tiles = [pieces[owner[0, k]] for k in range(slots)]
    weights = [arrival[0] * mult[0, k] for k in range(slots)]
    count = sum(w * t for w, t in zip(weights, tiles)).astype(jnp.float32)

    loads[0].wait()
    for k in range(slots):
        rows = pl.ds(k * tok, tok)
        Y[0, rows, :] = (cot[rows, :].astype(jnp.float32) * weights[k].astype(jnp.float32)).astype(jnp.bfloat16)
    Y[0, pl.ds(T, PAD), :] = jnp.full((PAD, Y.shape[2]), count, jnp.float32).astype(jnp.bfloat16)
    y_up = send(Y.at[0], Y.at[3], dev(dy=1))
    y_dn = send(Y.at[0], Y.at[1], dev(dy=-1))

    for q in range(nq):
        for r in range(NX):
            for k in range(NC):
                H[q][r, k, pl.ds(T, PAD), :] = jnp.zeros((PAD, WIDTHS[q]), jnp.bfloat16)

    loads[1].wait()
    loads[2].wait()

    def hidden(k, which, q):
        rows = pl.ds(k * tok, tok)
        cols = pl.ds(pl.multiple_of(which * half + offs[q], 128), WIDTHS[q])
        g = gate[rows, cols].astype(jnp.float32)
        u = lift[rows, cols].astype(jnp.float32)
        h = g / (1.0 + jnp.exp(-g)) * u
        row = lax.broadcasted_iota(jnp.int32, h.shape, 0)
        return jnp.where(row < tiles[k] * TILE, h, 0.0).astype(jnp.bfloat16)

    body = pl.ds(0, T)
    h_core, h_up, h_dn = {}, {}, {}

    def x_send(q, k):
        h_up[q, k] = send(H[q].at[0, k, body], H[q].at[3, k, body], dev(dx=1))
        h_dn[q, k] = send(H[q].at[0, k, body], H[q].at[1, k, body], dev(dx=-1))

    for q in range(nq):
        for k in range(slots):
            HS[q][pl.ds(k * tok, tok), :] = hidden(k, 1 - c, q)
        h_core[q] = send(HS[q], H[q].at[0, 1, body], dev(flip=True))
        for k in range(slots):
            H[q][0, 0, pl.ds(k * tok, tok), :] = hidden(k, c, q)
        if q < 2:
            x_send(q, 0)
        if q == 0:
            h_core[0].wait_recv()
            x_send(0, 1)

    y_up.wait_recv()
    y_fup = send(Y.at[3, pl.ds(LO, TP - LO)], Y.at[2, pl.ds(LO, TP - LO)], dev(dy=1))
    y_dn.wait_recv()
    y_fdn = send(Y.at[1, pl.ds(0, LO)], Y.at[2, pl.ds(0, LO)], dev(dy=-1))
    y_fup.wait_recv()
    y_fdn.wait_recv()

    far = (x + 2 + NY - y) % NY
    c_tu = send(Y.at[far, pl.ds(0, LO)], TU, dev(dx=1))
    c_td = send(Y.at[far, pl.ds(LO, TP - LO)], TD, dev(dx=-1))
    c_up = send(Y.at[(x + 1 + NY - y) % NY], C.at[3, 0], dev(dx=1))
    c_dn = send(Y.at[(x - 1 + NX + NY - y) % NY], C.at[1, 0], dev(dx=-1))
    mine = (x + NY - y) % NY
    c_core = {0: send(Y.at[mine], C.at[0, 1], dev(flip=True))}
    C[0, 0] = Y[mine]

    h_f = {}

    def forward(q):
        h_dn[q, 0].wait_recv()
        h_f[q, 0] = send(H[q].at[1, 0, body], H[q].at[2, 0, body], dev(dx=-1))
        h_up[q, 1].wait_recv()
        h_f[q, 1] = send(H[q].at[3, 1, body], H[q].at[2, 1, body], dev(dx=1))

    h_core[1].wait_recv()
    x_send(1, 1)
    c_tu.wait_recv()
    c_fu = send(TU, C.at[2, 0, pl.ds(0, LO)], dev(dx=1))
    c_td.wait_recv()
    c_fd = send(TD, C.at[2, 0, pl.ds(LO, TP - LO)], dev(dx=-1))
    forward(0)
    for q in range(2, nq):
        x_send(q, 0)
        h_core[q].wait_recv()
        x_send(q, 1)
    c_up.wait_recv()
    c_core[3] = send(C.at[3, 0], C.at[3, 1], dev(flip=True))
    c_dn.wait_recv()
    c_core[1] = send(C.at[1, 0], C.at[1, 1], dev(flip=True))
    forward(1)
    c_fu.wait_recv()
    c_fd.wait_recv()
    c_core[2] = send(C.at[2, 0], C.at[2, 1], dev(flip=True))
    for q in range(2, nq):
        forward(q)
    for r in range(NX):
        c_core[r].wait_recv()

    whole = C[...].reshape(NX * NC * TP, C.shape[3])
    CT[...] = whole.T
    cz = jnp.zeros((PAD, 128), jnp.float32)
    for r in range(NX):
        for k in range(NC):
            cz = cz + C[r, k, pl.ds(T, PAD), pl.ds(0, 128)].astype(jnp.float32)
    cnt_z[...] = cz

    base = []
    n = 0
    for _, dist in CHAINS:
        base.append(n)
        n += len(dist) - 1
    msgs = {}

    def z_step(q, s):
        for ci, (sign, dist) in enumerate(CHAINS):
            if s >= len(dist) - 1:
                continue
            slot = base[ci] + s
            own = (z + sign * dist[s] + nz) % nz
            to = dev(dz=sign * (dist[s] - dist[s + 1]))
            v = PR[q][own]
            if s > 0:
                msgs[q, ci, s - 1].wait_recv()
                v = v + ZR[q][slot - 1].astype(jnp.float32)
            ZS[q][slot] = v.astype(jnp.bfloat16)
            msgs[q, ci, s] = send(ZS[q].at[slot], ZR[q].at[slot], to)
            if q == 0:
                w = cnt_z[...]
                if s > 0:
                    msgs["c", ci, s - 1].wait_recv()
                    w = w + CR[slot - 1]
                CS[slot] = w
                msgs["c", ci, s] = send(CS.at[slot], CR.at[slot], to)

    steps = max(len(d) for _, d in CHAINS) - 1
    for t in range((nq - 1) * STAGGER + steps):
        for q in range(nq):
            s = t - q * STAGGER
            if s == 0:
                for d in (h_up[q, 0], h_dn[q, 1], h_f[q, 0], h_f[q, 1]):
                    d.wait_recv()
                rhs = H[q][...].reshape(NX * NC * TP, WIDTHS[q])
                for m in range(4):
                    acc = jnp.dot(CT[pl.ds(m * 128, 128), :], rhs, preferred_element_type=jnp.float32)
                    PR[q][pl.ds(m * (nz // 4), nz // 4)] = acc.reshape(nz // 4, 128 * 4 // nz, WIDTHS[q])
            if 0 <= s < steps:
                z_step(q, s)

    fin = {}
    total = cnt_z[...]
    for ci, (_, dist) in enumerate(CHAINS):
        msgs["c", ci, len(dist) - 2].wait_recv()
        total = total + CR[base[ci] + len(dist) - 2]
    total = total[0:1, 0:1] * float(TILE)
    for q in range(nq):
        v = PR[q][z]
        for ci, (_, dist) in enumerate(CHAINS):
            msgs[q, ci, len(dist) - 2].wait_recv()
            v = v + ZR[q][base[ci] + len(dist) - 2].astype(jnp.float32)
        R[q][...] = (v / total).reshape(R[q].shape)
        fin[q] = send(R[q].at[1 - c], FR[q], dev(flip=True))
        out[:, pl.ds(pl.multiple_of(c * half + offs[q], 128), WIDTHS[q])] = R[q][c]
    for q in range(nq):
        fin[q].wait_recv()
        out[:, pl.ds(pl.multiple_of((1 - c) * half + offs[q], 128), WIDTHS[q])] = FR[q][...]
    for d in every:
        d.wait_send()


def on_device(nz, gate, lift, cot, arrival, owner, mult, pieces):
    _, slots, tok, ff = gate.shape
    db = cot.shape[3]
    T, TP = slots * tok, slots * tok + PAD
    LO = (T // 2) // 16 * 16
    rows = db // nz
    n = sum(len(d) - 1 for _, d in CHAINS)
    bf, f32 = jnp.bfloat16, jnp.float32
    V = pltpu.VMEM
    any_ = pl.BlockSpec(memory_space=pl.ANY)
    smem = pl.BlockSpec(memory_space=pltpu.SMEM)
    return pl.pallas_call(
        functools.partial(kernel, nz, slots, tok),
        out_shape=jax.ShapeDtypeStruct((rows // NC, ff), f32),
        in_specs=[any_, any_, any_, smem, smem, smem, smem],
        out_specs=pl.BlockSpec(memory_space=pltpu.VMEM),
        scratch_shapes=[
            V((T, ff), bf), V((T, ff), bf), V((T, db), bf), pltpu.SemaphoreType.DMA((3,)),
            V((NY, TP, db), bf), V((LO, db), bf), V((TP - LO, db), bf),
            V((NX, NC, TP, db), bf), V((db, NX * NC * TP), bf),
            [V((NX, NC, TP, w), bf) for w in WIDTHS],
            [V((T, w), bf) for w in WIDTHS],
            [V((nz, rows, w), f32) for w in WIDTHS],
            [V((n, rows, w), bf) for w in WIDTHS],
            [V((n, rows, w), bf) for w in WIDTHS],
            V((n, PAD, 128), f32), V((n, PAD, 128), f32),
            [V((NC, rows // NC, w), f32) for w in WIDTHS],
            [V((rows // NC, w), f32) for w in WIDTHS],
            V((PAD, 128), f32),
            pltpu.SemaphoreType.DMA((SEMS,)), pltpu.SemaphoreType.DMA((SEMS,)),
        ],
        compiler_params=pltpu.CompilerParams(
            collective_id=0, has_side_effects=True, vmem_limit_bytes=60 * 1024 * 1024
        ),
    )(
        gate.reshape(T, ff), lift.reshape(T, ff), cot.reshape(T, db),
        arrival, owner, mult, pieces,
    )


def solution(mesh):
    nz = mesh.shape["dp"] // (NX * NC)
    return jax.shard_map(
        functools.partial(on_device, nz),
        mesh=mesh,
        in_specs=(
            P("dp", None, None, "mp"),
            P("dp", None, None, "mp"),
            P("dp", None, None, "mp"),
            P("dp"),
            P("dp", None),
            P("dp", None),
            P(),
        ),
        out_specs=P("dp", "mp"),
        check_vma=False,
    )
```

```python
import functools

import jax
import jax.numpy as jnp
from jax import lax
from jax.experimental import pallas as pl
from jax.experimental.pallas import tpu as pltpu
from jax.sharding import PartitionSpec as P

MESH = pl.DeviceIdType.MESH
TILE = 32
NX = 4
NY = 4
NC = 2
WIDTHS = (256, 256, 256, 128)
SKIP2 = ((-1, (8, 6, 4, 2, 0)), (1, (7, 5, 3, 1, 0)), (-1, (7, 5, 3, 1, 0)), (1, (6, 4, 2, 0)))
SKIP4 = (
    (-1, (8, 4, 0)), (1, (7, 3, 0)), (-1, (7, 3, 0)), (1, (6, 2, 0)),
    (-1, (6, 2, 0)), (1, (5, 1, 0)), (-1, (5, 1, 0)), (1, (4, 0)),
)
CHAINS = (SKIP2, SKIP2, SKIP2, SKIP4)
ORDER = (
    ("m", 0), ("z", 0, 0), ("m", 1), ("z", 1, 0), ("k", 0), ("f", 2), ("s", 3), ("z", 0, 1), ("z", 1, 1),
    ("m", 2), ("z", 2, 0), ("k", 0), ("f", 3), ("z", 0, 2), ("m", 3), ("z", 3, 0), ("z", 1, 2), ("z", 2, 1),
    ("k", 0), ("z", 0, 3), ("z", 1, 3), ("z", 3, 1), ("z", 2, 2), ("e", 0), ("e", 1), ("z", 3, 2), ("z", 2, 3),
    ("z", 3, 3), ("e", 2), ("e", 3),
)
COUNTS = (("c", 1, 1, 0), ("x", 1, 2, 1), ("z", 1, 1, 0), ("z", 2, 4, 3))
COUNT_MSGS = sum(up + down for _, _, up, down in COUNTS)
SENDS, RECVS = 80, 80


def kernel(
    nz, slots, tok,
    gate_hbm, lift_hbm, cot_hbm, arrival, owner, mult, pieces,
    out,
    gate, lift, cot, in_sem,
    W, B, C, CT, H, HS, PR, ZS, ZR, CS, CR, R, FR,
    ssem, rsem,
):
    T = slots * tok
    nq = len(WIDTHS)
    half = sum(WIDTHS)
    offs = [sum(WIDTHS[:q]) for q in range(nq)]
    part = T // NY
    low, high = pl.ds(0, NX // 2), pl.ds(NX // 2, NX // 2)

    dp = lax.axis_index("dp")
    y = lax.axis_index("mp")
    x = dp // (NC * nz)
    z = (dp // NC) % nz
    c = dp % NC

    def dev(dx=0, dy=0, dz=0, flip=False):
        xx = (x + dx + NX) % NX
        yy = (y + dy + NY) % NY
        zz = (z + dz + nz) % nz
        cc = 1 - c if flip else c
        return (xx * (NC * nz) + zz * NC + cc, yy)

    sids, rids = iter(range(SENDS)), iter(range(RECVS))
    every = []

    def copy(src, dst, to, i, j):
        return pltpu.make_async_remote_copy(
            src_ref=src, dst_ref=dst, send_sem=ssem.at[i], recv_sem=rsem.at[j],
            device_id=to, device_id_type=MESH,
        )

    def send(src, dst, to):
        d = copy(src, dst, to, next(sids), next(rids))
        d.start()
        every.append(d)
        return d

    loads = [
        pltpu.make_async_copy(cot_hbm, cot, in_sem.at[0]),
        pltpu.make_async_copy(gate_hbm, gate, in_sem.at[1]),
        pltpu.make_async_copy(lift_hbm, lift, in_sem.at[2]),
    ]
    for d in loads:
        d.start()

    near = [dev(flip=True)] + [dev(dx=d) for d in (1, 2, 3)] + [dev(dy=d) for d in (1, 2, 3)]
    for h in (1, 2):
        near += [dev(dz=h), dev(dz=-h)]
    barrier = pltpu.get_barrier_semaphore()
    for n in near:
        pl.semaphore_signal(barrier, inc=1, device_id=n, device_id_type=MESH)
    pl.semaphore_wait(barrier, len(near))

    tiles = [pieces[owner[0, k]] for k in range(slots)]
    weights = [arrival[0] * mult[0, k] for k in range(slots)]
    count = sum(w * t for w, t in zip(weights, tiles)).astype(jnp.float32)

    loads[0].wait()
    token = lax.broadcasted_iota(jnp.int32, (part, 1), 0)
    for t in range(NY):
        scale = jnp.zeros((part, 1), jnp.float32)
        for k in range(slots):
            here = (token + t * part >= k * tok) & (token + t * part < (k + 1) * tok)
            scale = jnp.where(here, weights[k].astype(jnp.float32), scale)
        W[t] = (cot[pl.ds(t * part, part), :].astype(jnp.float32) * scale).astype(jnp.bfloat16)
    b_sent = [
        send(W.at[(y + d) % NY], B.at[NY - d], dev(dy=d)) for d in (2, 1, 3)
    ]
    B[0] = W[y]

    def count_rounds():
        total = jnp.full((8, 128), count, jnp.float32)
        slot = 0
        for kind, hop, up, down in COUNTS:
            last = [total, total]
            got = [None, None]
            for step in range(max(up, down) + 1):
                for side, (sign, n) in enumerate(((1, up), (-1, down))):
                    if 0 < step <= n:
                        d, at = got[side]
                        d.wait_recv()
                        last[side] = CR[at] + (total if step < n else 0.0)
                    if step < n:
                        CS[slot] = last[side]
                        to = {"c": dev(flip=True), "x": dev(dx=sign * hop), "z": dev(dz=sign * hop)}[kind]
                        got[side] = (send(CS.at[slot], CR.at[slot], to), slot)
                        slot += 1
                if step < max(up, down):
                    yield
            total = total + last[0]
            if down:
                total = total + last[1]
        CS[slot] = total

    rounds = count_rounds()

    def count_step():
        next(rounds, None)

    count_step()
    loads[1].wait()
    loads[2].wait()

    def hidden(k, which, q):
        rows = pl.ds(k * tok, tok)
        cols = pl.ds(pl.multiple_of(which * half + offs[q], 128), WIDTHS[q])
        g = gate[rows, cols].astype(jnp.float32)
        u = lift[rows, cols].astype(jnp.float32)
        h = g / (1.0 + jnp.exp(-g)) * u
        row = lax.broadcasted_iota(jnp.int32, h.shape, 0)
        return jnp.where(row < tiles[k] * TILE, h, 0.0).astype(jnp.bfloat16)

    h_core, h_up, h_dn, h_f = {}, {}, {}, {}

    def x_send(q, k):
        if k == 1:
            h_core[q].wait_recv()
        h_up[q, k] = send(H[q].at[0, k], H[q].at[3, k], dev(dx=1))
        h_dn[q, k] = send(H[q].at[0, k], H[q].at[1, k], dev(dx=-1))

    def forward(q):
        h_dn[q, 0].wait_recv()
        h_f[q, 0] = send(H[q].at[1, 0], H[q].at[2, 0], dev(dx=-1))
        h_up[q, 1].wait_recv()
        h_f[q, 1] = send(H[q].at[3, 1], H[q].at[2, 1], dev(dx=1))

    for q in range(nq):
        for k in range(slots):
            HS[q][pl.ds(k * tok, tok), :] = hidden(k, 1 - c, q)
        h_core[q] = send(HS[q], H[q].at[0, 1], dev(flip=True))
        for k in range(slots):
            H[q][0, 0, pl.ds(k * tok, tok), :] = hidden(k, c, q)
        if q == 0:
            x_send(0, 0)
            x_send(0, 1)

    for d in b_sent:
        d.wait_recv()
    c_sent = [
        send(B.at[(x + d + NY - y) % NY], C.at[0, y, NX - d], dev(dx=d)) for d in (2, 1, 3)
    ]
    C[0, y, 0] = B[(x + NY - y) % NY]
    count_step()
    forward(0)
    x_send(1, 0)
    x_send(1, 1)
    for d in c_sent:
        d.wait_recv()
    count_step()

    def pair(rs, sign):
        i, j = next(sids), next(rids)
        to = dev(dy=sign)
        out = copy(C.at[0, y, rs], C.at[0, y, rs], to, i, j)
        out.start()
        t = (y - sign + NY) % NY
        every.append(out)
        return copy(C.at[0, t, rs], C.at[0, t, rs], to, i, j)

    q_u1 = pair(high, 1)
    q_d1 = pair(low, -1)
    q_u2 = pair(low, 1)
    q_d2 = pair(high, -1)
    before, after, across = (y + NY - 1) % NY, (y + 1) % NY, (y + 2) % NY

    core = []

    def to_core(t):
        core.append(send(C.at[0, t], C.at[1, t], dev(flip=True)))

    to_core(y)
    x_send(2, 0)
    x_send(2, 1)
    q_u1.wait_recv()
    i, j = next(sids), next(rids)
    out_u = copy(C.at[0, before, high], C.at[0, before, high], dev(dy=1), i, j)
    in_u = copy(C.at[0, across, high], C.at[0, across, high], dev(dy=1), i, j)
    out_u.start()
    q_d1.wait_recv()
    i, j = next(sids), next(rids)
    out_d = copy(C.at[0, after, low], C.at[0, after, low], dev(dy=-1), i, j)
    in_d = copy(C.at[0, across, low], C.at[0, across, low], dev(dy=-1), i, j)
    out_d.start()
    every += [out_u, out_d]
    count_step()
    forward(1)
    q_u2.wait_recv()
    to_core(before)
    q_d2.wait_recv()
    to_core(after)
    count_step()
    in_u.wait_recv()
    in_d.wait_recv()
    to_core(across)
    for d in core:
        d.wait_recv()
    pieces_ = [C[k, t, r] for r in range(NX) for k in range(NC) for t in range(NY)]
    CT[...] = jnp.concatenate(pieces_, axis=0).T

    def active(q, s):
        return sum(len(dist) - 1 > s for _, dist in CHAINS[q])

    zsem = {
        (q, s): (next(sids), next(rids))
        for q in range(nq) for s in range(len(CHAINS[q][0][1]) - 1)
    }

    def z_wait(q, s, recv):
        n = active(q, s)
        d = copy(ZS[q].at[s, pl.ds(0, n)], ZR[q].at[s, pl.ds(0, n)], dev(dz=1), *zsem[q, s])
        d.wait_recv() if recv else d.wait_send()

    def product(q):
        for d in (h_up[q, 0], h_dn[q, 1], h_f[q, 0], h_f[q, 1]):
            d.wait_recv()
        rhs = H[q][...].reshape(NX * NC * T, WIDTHS[q])
        for m in range(4):
            acc = jnp.dot(CT[pl.ds(m * 128, 128), :], rhs, preferred_element_type=jnp.float32)
            PR[q][pl.ds(m * (nz // 4), nz // 4)] = acc.reshape(nz // 4, 128 * 4 // nz, WIDTHS[q])

    def z_step(q, s):
        if s > 0:
            z_wait(q, s - 1, True)
        for ci in range(active(q, s)):
            sign, dist = CHAINS[q][ci]
            v = PR[q][(z + sign * dist[s] + nz) % nz]
            if s > 0:
                v = v + ZR[q][s - 1, ci].astype(jnp.float32)
            ZS[q][s, ci] = v.astype(jnp.bfloat16)
            to = dev(dz=sign * (dist[s] - dist[s + 1]))
            copy(ZS[q].at[s, ci], ZR[q].at[s, ci], to, *zsem[q, s]).start()

    fin = {}

    def end(q):
        for _ in rounds:
            pass
        steps = len(CHAINS[q][0][1]) - 1
        z_wait(q, steps - 1, True)
        v = PR[q][z]
        for ci, (_, dist) in enumerate(CHAINS[q]):
            v = v + ZR[q][len(dist) - 2, ci].astype(jnp.float32)
        total = CS[COUNT_MSGS][0:1, 0:1] * float(TILE)
        R[q][...] = (v / total).reshape(R[q].shape)
        fin[q] = send(R[q].at[1 - c], FR[q], dev(flip=True))
        out[:, pl.ds(pl.multiple_of(c * half + offs[q], 128), WIDTHS[q])] = R[q][c]

    for event in ORDER:
        q = event[1]
        if event[0] == "s":
            x_send(q, 0)
            x_send(q, 1)
        elif event[0] == "k":
            count_step()
        elif event[0] == "f":
            forward(q)
        elif event[0] == "m":
            product(q)
        elif event[0] == "z":
            if event[2] < len(CHAINS[q][0][1]) - 1:
                z_step(q, event[2])
        else:
            end(q)
    for q in range(nq):
        fin[q].wait_recv()
        out[:, pl.ds(pl.multiple_of((1 - c) * half + offs[q], 128), WIDTHS[q])] = FR[q][...]
    for d in every:
        d.wait_send()
    for q, s in zsem:
        z_wait(q, s, False)


def on_device(nz, gate, lift, cot, arrival, owner, mult, pieces):
    _, slots, tok, ff = gate.shape
    db = cot.shape[3]
    T = slots * tok
    rows = db // nz
    bf, f32 = jnp.bfloat16, jnp.float32
    V = pltpu.VMEM
    any_ = pl.BlockSpec(memory_space=pl.ANY)
    smem = pl.BlockSpec(memory_space=pltpu.SMEM)
    zbuf = [V((len(ch[0][1]) - 1, len(ch), rows, w), bf) for ch, w in zip(CHAINS, WIDTHS)]
    n = COUNT_MSGS
    return pl.pallas_call(
        functools.partial(kernel, nz, slots, tok),
        out_shape=jax.ShapeDtypeStruct((rows // NC, ff), f32),
        in_specs=[any_, any_, any_, smem, smem, smem, smem],
        out_specs=pl.BlockSpec(memory_space=pltpu.VMEM),
        scratch_shapes=[
            V((T, ff), bf), V((T, ff), bf), V((T, db), bf), pltpu.SemaphoreType.DMA((3,)),
            V((NY, T // NY, db), bf), V((NY, T // NY, db), bf),
            V((NC, NY, NX, T // NY, db), bf), V((db, NX * NC * T), bf),
            [V((NX, NC, T, w), bf) for w in WIDTHS],
            [V((T, w), bf) for w in WIDTHS],
            [V((nz, rows, w), f32) for w in WIDTHS],
            zbuf, list(zbuf),
            V((n + 1, 8, 128), f32), V((n, 8, 128), f32),
            [V((NC, rows // NC, w), f32) for w in WIDTHS],
            [V((rows // NC, w), f32) for w in WIDTHS],
            pltpu.SemaphoreType.DMA((SENDS,)), pltpu.SemaphoreType.DMA((RECVS,)),
        ],
        compiler_params=pltpu.CompilerParams(
            collective_id=0, has_side_effects=True, vmem_limit_bytes=60 * 1024 * 1024
        ),
    )(
        gate.reshape(T, ff), lift.reshape(T, ff), cot.reshape(T, db),
        arrival, owner, mult, pieces,
    )


def solution(mesh):
    nz = mesh.shape["dp"] // (NX * NC)
    return jax.shard_map(
        functools.partial(on_device, nz),
        mesh=mesh,
        in_specs=(
            P("dp", None, None, "mp"),
            P("dp", None, None, "mp"),
            P("dp", None, None, "mp"),
            P("dp"),
            P("dp", None),
            P("dp", None),
            P(),
        ),
        out_specs=P("dp", "mp"),
        check_vma=False,
    )
```

```python
import functools

import jax
import jax.numpy as jnp
from jax import lax
from jax.experimental import pallas as pl
from jax.experimental.pallas import tpu as pltpu
from jax.sharding import PartitionSpec as P

MESH = pl.DeviceIdType.MESH
TILE = 32
NX = 4
NY = 4
NC = 2
WIDTHS = (256, 256, 256, 128)
BOTH = (1, -1)
LEAVES = tuple((g, d, d - 1) for d in (7, 5, 3, 1) for g in BOTH)
TREE2 = (
    (0, LEAVES), (0, ((-1, 8, 6),)), (1, ((1, 6, 4), (-1, 6, 4))), (2, ((1, 4, 2), (-1, 4, 2))),
    (3, ((1, 2, 0), (-1, 2, 0))),
)
TREE4 = (
    (0, LEAVES), (0, ((-1, 8, 4),)), (1, ((1, 6, 4), (-1, 6, 4), (1, 2, 0), (-1, 2, 0))), (2, ((1, 4, 0), (-1, 4, 0))),
)
TREES = (TREE2, TREE2, TREE4, TREE4)
ORDER = (
    ("m", 0), ("z", 0, 0), ("f", 2), ("k", 0), ("m", 1), ("z", 1, 0), ("z", 0, 1), ("f", 3), ("z", 0, 2), ("k", 0),
    ("z", 1, 1), ("m", 2), ("z", 2, 0), ("m", 3), ("z", 3, 0), ("k", 0), ("z", 0, 3), ("z", 2, 1), ("z", 1, 2),
    ("z", 3, 1), ("e", 0), ("z", 2, 2), ("z", 1, 3), ("z", 3, 2), ("e", 1), ("e", 2), ("e", 3),
)
COUNTS = (("c", 1, 1, 0), ("x", 1, 2, 1), ("z", 1, 1, 0), ("z", 2, 4, 3))
COUNT_MSGS = sum(up + down for _, _, up, down in COUNTS)
SENDS, RECVS = 80, 80


def kernel(
    nz, slots, tok,
    gate_hbm, lift_hbm, cot_hbm, arrival, owner, mult, pieces,
    out,
    gate, lift, cot, in_sem,
    W, B, C, CT, H, HS, PR, ZS, ZR, CS, CR, R, out_sem,
    ssem, rsem,
):
    T = slots * tok
    nq = len(WIDTHS)
    half = sum(WIDTHS)
    offs = [sum(WIDTHS[:q]) for q in range(nq)]
    part = T // NY
    low, high = pl.ds(0, NX // 2), pl.ds(NX // 2, NX // 2)

    dp = lax.axis_index("dp")
    y = lax.axis_index("mp")
    x = dp // (NC * nz)
    z = (dp // NC) % nz
    c = dp % NC

    def dev(dx=0, dy=0, dz=0, flip=False):
        xx = (x + dx + NX) % NX
        yy = (y + dy + NY) % NY
        zz = (z + dz + nz) % nz
        cc = 1 - c if flip else c
        return (xx * (NC * nz) + zz * NC + cc, yy)

    sids, rids = iter(range(SENDS)), iter(range(RECVS))
    every = []

    def copy(src, dst, to, i, j):
        return pltpu.make_async_remote_copy(
            src_ref=src, dst_ref=dst, send_sem=ssem.at[i], recv_sem=rsem.at[j],
            device_id=to, device_id_type=MESH,
        )

    def send(src, dst, to):
        d = copy(src, dst, to, next(sids), next(rids))
        d.start()
        every.append(d)
        return d

    loads = [
        pltpu.make_async_copy(cot_hbm, cot, in_sem.at[0]),
        pltpu.make_async_copy(gate_hbm, gate, in_sem.at[1]),
        pltpu.make_async_copy(lift_hbm, lift, in_sem.at[2]),
    ]
    for d in loads:
        d.start()

    near = [dev(flip=True)] + [dev(dx=d) for d in (1, 2, 3)] + [dev(dy=d) for d in (1, 2, 3)]
    for h in (1, 2):
        near += [dev(dz=h), dev(dz=-h)]
    barrier = pltpu.get_barrier_semaphore()
    for n in near:
        pl.semaphore_signal(barrier, inc=1, device_id=n, device_id_type=MESH)
    pl.semaphore_wait(barrier, len(near))

    tiles = [pieces[owner[0, k]] for k in range(slots)]
    weights = [arrival[0] * mult[0, k] for k in range(slots)]
    count = sum(w * t for w, t in zip(weights, tiles)).astype(jnp.float32)

    loads[0].wait()
    token = lax.broadcasted_iota(jnp.int32, (part, 1), 0)
    for t in range(NY):
        scale = jnp.zeros((part, 1), jnp.float32)
        for k in range(slots):
            here = (token + t * part >= k * tok) & (token + t * part < (k + 1) * tok)
            scale = jnp.where(here, weights[k].astype(jnp.float32), scale)
        W[t] = (cot[pl.ds(t * part, part), :].astype(jnp.float32) * scale).astype(jnp.bfloat16)
    b_sent = [
        send(W.at[(y + d) % NY], B.at[NY - d], dev(dy=d)) for d in (2, 1, 3)
    ]
    B[0] = W[y]

    def count_rounds():
        total = jnp.full((8, 128), count, jnp.float32)
        slot = 0
        for kind, hop, up, down in COUNTS:
            last = [total, total]
            got = [None, None]
            for step in range(max(up, down) + 1):
                for side, (sign, n) in enumerate(((1, up), (-1, down))):
                    if 0 < step <= n:
                        d, at = got[side]
                        d.wait_recv()
                        last[side] = CR[at] + (total if step < n else 0.0)
                    if step < n:
                        CS[slot] = last[side]
                        to = {"c": dev(flip=True), "x": dev(dx=sign * hop), "z": dev(dz=sign * hop)}[kind]
                        got[side] = (send(CS.at[slot], CR.at[slot], to), slot)
                        slot += 1
                if step < max(up, down):
                    yield
            total = total + last[0]
            if down:
                total = total + last[1]
        CS[slot] = total

    rounds = count_rounds()

    def count_step():
        next(rounds, None)

    count_step()
    loads[1].wait()
    loads[2].wait()

    def hidden(k, which, q):
        rows = pl.ds(k * tok, tok)
        cols = pl.ds(pl.multiple_of(which * half + offs[q], 128), WIDTHS[q])
        g = gate[rows, cols].astype(jnp.float32)
        u = lift[rows, cols].astype(jnp.float32)
        h = g / (1.0 + jnp.exp(-g)) * u
        row = lax.broadcasted_iota(jnp.int32, h.shape, 0)
        return jnp.where(row < tiles[k] * TILE, h, 0.0).astype(jnp.bfloat16)

    h_core, h_up, h_dn, h_f = {}, {}, {}, {}

    def x_send(q, k):
        if k == 1:
            h_core[q].wait_recv()
        h_up[q, k] = send(H[q].at[0, k], H[q].at[3, k], dev(dx=1))
        h_dn[q, k] = send(H[q].at[0, k], H[q].at[1, k], dev(dx=-1))

    def forward(q):
        h_dn[q, 0].wait_recv()
        h_f[q, 0] = send(H[q].at[1, 0], H[q].at[2, 0], dev(dx=-1))
        h_up[q, 1].wait_recv()
        h_f[q, 1] = send(H[q].at[3, 1], H[q].at[2, 1], dev(dx=1))

    for q in range(nq):
        for k in range(slots):
            HS[q][pl.ds(k * tok, tok), :] = hidden(k, 1 - c, q)
        h_core[q] = send(HS[q], H[q].at[0, 1], dev(flip=True))
        for k in range(slots):
            H[q][0, 0, pl.ds(k * tok, tok), :] = hidden(k, c, q)
        if q == 0:
            x_send(0, 0)
            x_send(0, 1)

    for d in b_sent:
        d.wait_recv()
    c_sent = [
        send(B.at[(x + d + NY - y) % NY], C.at[0, y, NX - d], dev(dx=d)) for d in (2, 1, 3)
    ]
    C[0, y, 0] = B[(x + NY - y) % NY]
    count_step()
    forward(0)
    x_send(1, 0)
    x_send(1, 1)
    for d in c_sent:
        d.wait_recv()
    count_step()

    def pair(rs, sign):
        i, j = next(sids), next(rids)
        to = dev(dy=sign)
        out = copy(C.at[0, y, rs], C.at[0, y, rs], to, i, j)
        out.start()
        t = (y - sign + NY) % NY
        every.append(out)
        return copy(C.at[0, t, rs], C.at[0, t, rs], to, i, j)

    q_u1 = pair(high, 1)
    q_d1 = pair(low, -1)
    q_u2 = pair(low, 1)
    q_d2 = pair(high, -1)
    before, after, across = (y + NY - 1) % NY, (y + 1) % NY, (y + 2) % NY

    core = []

    def to_core(t):
        core.append(send(C.at[0, t], C.at[1, t], dev(flip=True)))

    to_core(y)
    x_send(2, 0)
    x_send(2, 1)
    q_u1.wait_recv()
    i, j = next(sids), next(rids)
    out_u = copy(C.at[0, before, high], C.at[0, before, high], dev(dy=1), i, j)
    in_u = copy(C.at[0, across, high], C.at[0, across, high], dev(dy=1), i, j)
    out_u.start()
    q_d1.wait_recv()
    i, j = next(sids), next(rids)
    out_d = copy(C.at[0, after, low], C.at[0, after, low], dev(dy=-1), i, j)
    in_d = copy(C.at[0, across, low], C.at[0, across, low], dev(dy=-1), i, j)
    out_d.start()
    every += [out_u, out_d]
    count_step()
    forward(1)
    x_send(3, 0)
    x_send(3, 1)
    q_u2.wait_recv()
    to_core(before)
    q_d2.wait_recv()
    to_core(after)
    count_step()
    in_u.wait_recv()
    in_d.wait_recv()
    to_core(across)
    for d in core:
        d.wait_recv()
    pieces_ = [C[k, t, r] for r in range(NX) for k in range(NC) for t in range(NY)]
    CT[...] = jnp.concatenate(pieces_, axis=0).T

    zsem = {(q, g): (next(sids), next(rids)) for q in range(nq) for g in range(len(TREES[q]))}
    first = {}
    for q in range(nq):
        n = 0
        for g, (_, group) in enumerate(TREES[q]):
            first[q, g] = n
            n += len(group)
    waited = set()

    def z_group(q, g):
        at = pl.ds(first[q, g], len(TREES[q][g][1]))
        return copy(ZS[q].at[at], ZR[q].at[at], dev(dz=1), *zsem[q, g])

    def z_sum(q, sign, dist):
        v = PR[q][(z + sign * dist + nz) % nz]
        for g, (_, group) in enumerate(TREES[q]):
            for i, (way, _, to) in enumerate(group):
                if to == dist and (way == sign or dist == 0):
                    if (q, g) not in waited:
                        waited.add((q, g))
                        z_group(q, g).wait_recv()
                    v = v + ZR[q][first[q, g] + i].astype(jnp.float32)
        return v

    def product(q):
        for d in (h_up[q, 0], h_dn[q, 1], h_f[q, 0], h_f[q, 1]):
            d.wait_recv()
        rhs = H[q][...].reshape(NX * NC * T, WIDTHS[q])
        for m in range(4):
            acc = jnp.dot(CT[pl.ds(m * 128, 128), :], rhs, preferred_element_type=jnp.float32)
            PR[q][pl.ds(m * (nz // 4), nz // 4)] = acc.reshape(nz // 4, 128 * 4 // nz, WIDTHS[q])

    def z_step(q, s):
        for g, (step, group) in enumerate(TREES[q]):
            if step == s:
                for i, (sign, dist, to) in enumerate(group):
                    slot = first[q, g] + i
                    ZS[q][slot] = z_sum(q, sign, dist).astype(jnp.bfloat16)
                    copy(ZS[q].at[slot], ZR[q].at[slot], dev(dz=sign * (dist - to)), *zsem[q, g]).start()

    fin = []

    def end(q):
        for _ in rounds:
            pass
        total = CS[COUNT_MSGS][0:1, 0:1] * float(TILE)
        R[q][...] = (z_sum(q, 1, 0) / total).reshape(R[q].shape)
        cols = out.at[:, pl.ds(pl.multiple_of(c * half + offs[q], 128), WIDTHS[q])]
        theirs = out.at[:, pl.ds(pl.multiple_of((1 - c) * half + offs[q], 128), WIDTHS[q])]
        i, j = next(sids), next(rids)
        d = copy(R[q].at[1 - c], cols, dev(flip=True), i, j)
        d.start()
        every.append(d)
        fin.append(copy(R[q].at[1 - c], theirs, dev(flip=True), i, j).wait_recv)
        d = pltpu.make_async_copy(R[q].at[c], cols, out_sem.at[q])
        d.start()
        fin.append(d.wait)

    for event in ORDER:
        q = event[1]
        if event[0] == "s":
            x_send(q, 0)
            x_send(q, 1)
        elif event[0] == "k":
            count_step()
        elif event[0] == "f":
            forward(q)
        elif event[0] == "m":
            product(q)
        elif event[0] == "z":
            z_step(q, event[2])
        else:
            end(q)
    for wait in fin:
        wait()
    for d in every:
        d.wait_send()
    for q, g in zsem:
        z_group(q, g).wait_send()


def on_device(nz, gate, lift, cot, arrival, owner, mult, pieces):
    _, slots, tok, ff = gate.shape
    db = cot.shape[3]
    T = slots * tok
    rows = db // nz
    bf, f32 = jnp.bfloat16, jnp.float32
    V = pltpu.VMEM
    any_ = pl.BlockSpec(memory_space=pl.ANY)
    smem = pl.BlockSpec(memory_space=pltpu.SMEM)
    zbuf = [V((sum(len(g) for _, g in tree), rows, w), bf) for tree, w in zip(TREES, WIDTHS)]
    n = COUNT_MSGS
    return pl.pallas_call(
        functools.partial(kernel, nz, slots, tok),
        out_shape=jax.ShapeDtypeStruct((rows // NC, ff), f32),
        in_specs=[any_, any_, any_, smem, smem, smem, smem],
        out_specs=any_,
        scratch_shapes=[
            V((T, ff), bf), V((T, ff), bf), V((T, db), bf), pltpu.SemaphoreType.DMA((3,)),
            V((NY, T // NY, db), bf), V((NY, T // NY, db), bf),
            V((NC, NY, NX, T // NY, db), bf), V((db, NX * NC * T), bf),
            [V((NX, NC, T, w), bf) for w in WIDTHS],
            [V((T, w), bf) for w in WIDTHS],
            [V((nz, rows, w), f32) for w in WIDTHS],
            zbuf, list(zbuf),
            V((n + 1, 8, 128), f32), V((n, 8, 128), f32),
            [V((NC, rows // NC, w), f32) for w in WIDTHS],
            pltpu.SemaphoreType.DMA((len(WIDTHS),)),
            pltpu.SemaphoreType.DMA((SENDS,)), pltpu.SemaphoreType.DMA((RECVS,)),
        ],
        compiler_params=pltpu.CompilerParams(
            collective_id=0, has_side_effects=True, vmem_limit_bytes=60 * 1024 * 1024
        ),
    )(
        gate.reshape(T, ff), lift.reshape(T, ff), cot.reshape(T, db),
        arrival, owner, mult, pieces,
    )


def solution(mesh):
    nz = mesh.shape["dp"] // (NX * NC)
    return jax.shard_map(
        functools.partial(on_device, nz),
        mesh=mesh,
        in_specs=(
            P("dp", None, None, "mp"),
            P("dp", None, None, "mp"),
            P("dp", None, None, "mp"),
            P("dp"),
            P("dp", None),
            P("dp", None),
            P(),
        ),
        out_specs=P("dp", "mp"),
        check_vma=False,
    )
```

```python
import functools

import jax
import jax.numpy as jnp
from jax import lax
from jax.experimental import pallas as pl
from jax.experimental.pallas import tpu as pltpu
from jax.sharding import PartitionSpec as P

MESH = pl.DeviceIdType.MESH
TILE = 32
NX = 4
NY = 4
NC = 2
WIDTHS = (256, 256, 256, 128)
BOTH = (1, -1)
LEAVES = tuple((g, d, d - 1) for d in (7, 5, 3, 1) for g in BOTH)
TREE2 = (
    (0, LEAVES), (0, ((-1, 8, 6),)), (1, ((1, 6, 4), (-1, 6, 4))), (2, ((1, 4, 2), (-1, 4, 2))),
    (3, ((1, 2, 0), (-1, 2, 0))),
)
TREE4 = (
    (0, LEAVES), (0, ((-1, 8, 4),)), (1, ((1, 6, 4), (-1, 6, 4), (1, 2, 0), (-1, 2, 0))), (2, ((1, 4, 0), (-1, 4, 0))),
)
TREES = (TREE2, TREE2, TREE4, TREE4)
ORDER = (
    ("m", 0), ("z", 0, 0), ("f", 2), ("k", 0), ("m", 1), ("z", 1, 0), ("z", 0, 1), ("f", 3), ("z", 0, 2), ("k", 0),
    ("z", 1, 1), ("m", 2), ("z", 2, 0), ("m", 3), ("z", 3, 0), ("k", 0), ("z", 0, 3), ("z", 2, 1), ("z", 1, 2),
    ("z", 3, 1), ("e", 0), ("z", 2, 2), ("z", 1, 3), ("z", 3, 2), ("e", 1), ("e", 2), ("e", 3),
)
COUNTS = (("c", 1, 1, 0), ("x", 1, 2, 1), ("z", 1, 1, 0), ("z", 2, 4, 3))
COUNT_MSGS = sum(up + down for _, _, up, down in COUNTS)
SENDS, RECVS = 80, 80


def kernel(
    nz, slots, tok,
    gate_hbm, lift_hbm, cot_hbm, arrival, owner, mult, pieces,
    out,
    gate, lift, cot, in_sem,
    W, B, C, CT, H, HS, PR, ZS, ZR, CS, CR, R, out_sem,
    ssem, rsem,
):
    T = slots * tok
    nq = len(WIDTHS)
    half = sum(WIDTHS)
    offs = [sum(WIDTHS[:q]) for q in range(nq)]
    part = T // NY
    low, high = pl.ds(0, NX // 2), pl.ds(NX // 2, NX // 2)

    dp = lax.axis_index("dp")
    y = lax.axis_index("mp")
    x = dp // (NC * nz)
    z = (dp // NC) % nz
    c = dp % NC
    turn = 1 - 2 * c

    def dev(dx=0, dy=0, dz=0, flip=False):
        xx = (x + dx + NX) % NX
        yy = (y + dy + NY) % NY
        zz = (z + dz + nz) % nz
        cc = 1 - c if flip else c
        return (xx * (NC * nz) + zz * NC + cc, yy)

    sids, rids = iter(range(SENDS)), iter(range(RECVS))
    every = []

    def copy(src, dst, to, i, j):
        return pltpu.make_async_remote_copy(
            src_ref=src, dst_ref=dst, send_sem=ssem.at[i], recv_sem=rsem.at[j],
            device_id=to, device_id_type=MESH,
        )

    def send(src, dst, to):
        d = copy(src, dst, to, next(sids), next(rids))
        d.start()
        every.append(d)
        return d

    loads = [
        pltpu.make_async_copy(cot_hbm, cot, in_sem.at[0]),
        pltpu.make_async_copy(gate_hbm, gate, in_sem.at[1]),
        pltpu.make_async_copy(lift_hbm, lift, in_sem.at[2]),
    ]
    for d in loads:
        d.start()

    near = [dev(flip=True)] + [dev(dx=d) for d in (1, 2, 3)] + [dev(dy=d) for d in (1, 2, 3)]
    for h in (1, 2):
        near += [dev(dz=h), dev(dz=-h)]
    barrier = pltpu.get_barrier_semaphore()
    for n in near:
        pl.semaphore_signal(barrier, inc=1, device_id=n, device_id_type=MESH)
    pl.semaphore_wait(barrier, len(near))

    tiles = [pieces[owner[0, k]] for k in range(slots)]
    weights = [arrival[0] * mult[0, k] for k in range(slots)]
    count = sum(w * t for w, t in zip(weights, tiles)).astype(jnp.float32)

    loads[0].wait()
    token = lax.broadcasted_iota(jnp.int32, (part, 1), 0)
    for t in range(NY):
        scale = jnp.zeros((part, 1), jnp.float32)
        for k in range(slots):
            here = (token + t * part >= k * tok) & (token + t * part < (k + 1) * tok)
            scale = jnp.where(here, weights[k].astype(jnp.float32), scale)
        W[t] = (cot[pl.ds(t * part, part), :].astype(jnp.float32) * scale).astype(jnp.bfloat16)
    b_sent = [
        send(W.at[(y + d) % NY], B.at[NY - d], dev(dy=d)) for d in (2, 1, 3)
    ]
    B[0] = W[y]

    def count_rounds():
        total = jnp.full((8, 128), count, jnp.float32)
        slot = 0
        for kind, hop, up, down in COUNTS:
            last = [total, total]
            got = [None, None]
            for step in range(max(up, down) + 1):
                for side, (sign, n) in enumerate(((1, up), (-1, down))):
                    if 0 < step <= n:
                        d, at = got[side]
                        d.wait_recv()
                        last[side] = CR[at] + (total if step < n else 0.0)
                    if step < n:
                        CS[slot] = last[side]
                        to = {"c": dev(flip=True), "x": dev(dx=sign * hop), "z": dev(dz=sign * hop)}[kind]
                        got[side] = (send(CS.at[slot], CR.at[slot], to), slot)
                        slot += 1
                if step < max(up, down):
                    yield
            total = total + last[0]
            if down:
                total = total + last[1]
        CS[slot] = total

    rounds = count_rounds()

    def count_step():
        next(rounds, None)

    count_step()
    loads[1].wait()
    loads[2].wait()

    def hidden(k, which, q):
        rows = pl.ds(k * tok, tok)
        cols = pl.ds(pl.multiple_of(which * half + offs[q], 128), WIDTHS[q])
        g = gate[rows, cols].astype(jnp.float32)
        u = lift[rows, cols].astype(jnp.float32)
        h = g / (1.0 + jnp.exp(-g)) * u
        row = lax.broadcasted_iota(jnp.int32, h.shape, 0)
        return jnp.where(row < tiles[k] * TILE, h, 0.0).astype(jnp.bfloat16)

    h_core, h_up, h_dn, h_f = {}, {}, {}, {}

    def x_send(q, k):
        if k == 1:
            h_core[q].wait_recv()
        h_up[q, k] = send(H[q].at[0, k], H[q].at[3, k], dev(dx=1))
        h_dn[q, k] = send(H[q].at[0, k], H[q].at[1, k], dev(dx=-1))

    def forward(q):
        h_dn[q, 0].wait_recv()
        h_f[q, 0] = send(H[q].at[1, 0], H[q].at[2, 0], dev(dx=-1))
        h_up[q, 1].wait_recv()
        h_f[q, 1] = send(H[q].at[3, 1], H[q].at[2, 1], dev(dx=1))

    for q in range(nq):
        for k in range(slots):
            HS[q][pl.ds(k * tok, tok), :] = hidden(k, 1 - c, q)
        h_core[q] = send(HS[q], H[q].at[0, 1], dev(flip=True))
        for k in range(slots):
            H[q][0, 0, pl.ds(k * tok, tok), :] = hidden(k, c, q)
        if q == 0:
            x_send(0, 0)
            x_send(0, 1)

    for d in b_sent:
        d.wait_recv()
    c_sent = [
        send(B.at[(x + d + NY - y) % NY], C.at[0, y, NX - d], dev(dx=d)) for d in (2, 1, 3)
    ]
    C[0, y, 0] = B[(x + NY - y) % NY]
    count_step()
    forward(0)
    x_send(1, 0)
    x_send(1, 1)
    for d in c_sent:
        d.wait_recv()
    count_step()

    def pair(rs, sign):
        i, j = next(sids), next(rids)
        to = dev(dy=sign)
        out = copy(C.at[0, y, rs], C.at[0, y, rs], to, i, j)
        out.start()
        t = (y - sign + NY) % NY
        every.append(out)
        return copy(C.at[0, t, rs], C.at[0, t, rs], to, i, j)

    q_u1 = pair(high, 1)
    q_d1 = pair(low, -1)
    q_u2 = pair(low, 1)
    q_d2 = pair(high, -1)
    before, after, across = (y + NY - 1) % NY, (y + 1) % NY, (y + 2) % NY

    core = []

    def to_core(t):
        core.append(send(C.at[0, t], C.at[1, t], dev(flip=True)))

    to_core(y)
    x_send(2, 0)
    x_send(2, 1)
    q_u1.wait_recv()
    i, j = next(sids), next(rids)
    out_u = copy(C.at[0, before, high], C.at[0, before, high], dev(dy=1), i, j)
    in_u = copy(C.at[0, across, high], C.at[0, across, high], dev(dy=1), i, j)
    out_u.start()
    q_d1.wait_recv()
    i, j = next(sids), next(rids)
    out_d = copy(C.at[0, after, low], C.at[0, after, low], dev(dy=-1), i, j)
    in_d = copy(C.at[0, across, low], C.at[0, across, low], dev(dy=-1), i, j)
    out_d.start()
    every += [out_u, out_d]
    count_step()
    forward(1)
    x_send(3, 0)
    x_send(3, 1)
    q_u2.wait_recv()
    to_core(before)
    q_d2.wait_recv()
    to_core(after)
    count_step()
    in_u.wait_recv()
    in_d.wait_recv()
    to_core(across)
    for d in core:
        d.wait_recv()
    pieces_ = [C[k, t, r] for r in range(NX) for k in range(NC) for t in range(NY)]
    CT[...] = jnp.concatenate(pieces_, axis=0).T

    zsem = {(q, g): (next(sids), next(rids)) for q in range(nq) for g in range(len(TREES[q]))}
    first = {}
    for q in range(nq):
        n = 0
        for g, (_, group) in enumerate(TREES[q]):
            first[q, g] = n
            n += len(group)
    waited = set()

    def z_group(q, g):
        at = pl.ds(first[q, g], len(TREES[q][g][1]))
        return copy(ZS[q].at[at], ZR[q].at[at], dev(dz=1), *zsem[q, g])

    def z_sum(q, sign, dist):
        v = PR[q][(z + turn * sign * dist + nz) % nz]
        for g, (_, group) in enumerate(TREES[q]):
            for i, (way, _, to) in enumerate(group):
                if to == dist and (way == sign or dist == 0):
                    if (q, g) not in waited:
                        waited.add((q, g))
                        z_group(q, g).wait_recv()
                    v = v + ZR[q][first[q, g] + i].astype(jnp.float32)
        return v

    def product(q):
        for d in (h_up[q, 0], h_dn[q, 1], h_f[q, 0], h_f[q, 1]):
            d.wait_recv()
        rhs = H[q][...].reshape(NX * NC * T, WIDTHS[q])
        for m in range(4):
            acc = jnp.dot(CT[pl.ds(m * 128, 128), :], rhs, preferred_element_type=jnp.float32)
            PR[q][pl.ds(m * (nz // 4), nz // 4)] = acc.reshape(nz // 4, 128 * 4 // nz, WIDTHS[q])

    def z_step(q, s):
        for g, (step, group) in enumerate(TREES[q]):
            if step == s:
                for i, (sign, dist, to) in enumerate(group):
                    slot = first[q, g] + i
                    ZS[q][slot] = z_sum(q, sign, dist).astype(jnp.bfloat16)
                    copy(ZS[q].at[slot], ZR[q].at[slot], dev(dz=turn * sign * (dist - to)), *zsem[q, g]).start()

    fin = []

    def end(q):
        for _ in rounds:
            pass
        total = CS[COUNT_MSGS][0:1, 0:1] * float(TILE)
        R[q][...] = (z_sum(q, 1, 0) / total).reshape(R[q].shape)
        cols = out.at[:, pl.ds(pl.multiple_of(c * half + offs[q], 128), WIDTHS[q])]
        theirs = out.at[:, pl.ds(pl.multiple_of((1 - c) * half + offs[q], 128), WIDTHS[q])]
        i, j = next(sids), next(rids)
        d = copy(R[q].at[1 - c], cols, dev(flip=True), i, j)
        d.start()
        every.append(d)
        fin.append(copy(R[q].at[1 - c], theirs, dev(flip=True), i, j).wait_recv)
        d = pltpu.make_async_copy(R[q].at[c], cols, out_sem.at[q])
        d.start()
        fin.append(d.wait)

    for event in ORDER:
        q = event[1]
        if event[0] == "s":
            x_send(q, 0)
            x_send(q, 1)
        elif event[0] == "k":
            count_step()
        elif event[0] == "f":
            forward(q)
        elif event[0] == "m":
            product(q)
        elif event[0] == "z":
            z_step(q, event[2])
        else:
            end(q)
    for wait in fin:
        wait()
    for d in every:
        d.wait_send()
    for q, g in zsem:
        z_group(q, g).wait_send()


def on_device(nz, gate, lift, cot, arrival, owner, mult, pieces):
    _, slots, tok, ff = gate.shape
    db = cot.shape[3]
    T = slots * tok
    rows = db // nz
    bf, f32 = jnp.bfloat16, jnp.float32
    V = pltpu.VMEM
    any_ = pl.BlockSpec(memory_space=pl.ANY)
    smem = pl.BlockSpec(memory_space=pltpu.SMEM)
    zbuf = [V((sum(len(g) for _, g in tree), rows, w), bf) for tree, w in zip(TREES, WIDTHS)]
    n = COUNT_MSGS
    return pl.pallas_call(
        functools.partial(kernel, nz, slots, tok),
        out_shape=jax.ShapeDtypeStruct((rows // NC, ff), f32),
        in_specs=[any_, any_, any_, smem, smem, smem, smem],
        out_specs=any_,
        scratch_shapes=[
            V((T, ff), bf), V((T, ff), bf), V((T, db), bf), pltpu.SemaphoreType.DMA((3,)),
            V((NY, T // NY, db), bf), V((NY, T // NY, db), bf),
            V((NC, NY, NX, T // NY, db), bf), V((db, NX * NC * T), bf),
            [V((NX, NC, T, w), bf) for w in WIDTHS],
            [V((T, w), bf) for w in WIDTHS],
            [V((nz, rows, w), f32) for w in WIDTHS],
            zbuf, list(zbuf),
            V((n + 1, 8, 128), f32), V((n, 8, 128), f32),
            [V((NC, rows // NC, w), f32) for w in WIDTHS],
            pltpu.SemaphoreType.DMA((len(WIDTHS),)),
            pltpu.SemaphoreType.DMA((SENDS,)), pltpu.SemaphoreType.DMA((RECVS,)),
        ],
        compiler_params=pltpu.CompilerParams(
            collective_id=0, has_side_effects=True, vmem_limit_bytes=60 * 1024 * 1024
        ),
    )(
        gate.reshape(T, ff), lift.reshape(T, ff), cot.reshape(T, db),
        arrival, owner, mult, pieces,
    )


def solution(mesh):
    nz = mesh.shape["dp"] // (NX * NC)
    return jax.shard_map(
        functools.partial(on_device, nz),
        mesh=mesh,
        in_specs=(
            P("dp", None, None, "mp"),
            P("dp", None, None, "mp"),
            P("dp", None, None, "mp"),
            P("dp"),
            P("dp", None),
            P("dp", None),
            P(),
        ),
        out_specs=P("dp", "mp"),
        check_vma=False,
    )
```

```python
import functools

import jax
import jax.numpy as jnp
from jax import lax
from jax.experimental import pallas as pl
from jax.experimental.pallas import tpu as pltpu
from jax.sharding import PartitionSpec as P

MESH = pl.DeviceIdType.MESH
TILE = 32
NX = 4
NY = 4
NC = 2
WIDTHS = (256, 256, 256, 128)
BOTH = (1, -1)
LEAVES = tuple((g, d, d - 1) for d in (7, 5, 3, 1) for g in BOTH)
TREE2 = (
    (0, LEAVES), (0, ((-1, 8, 6),)), (1, ((1, 6, 4), (-1, 6, 4))), (2, ((1, 4, 2), (-1, 4, 2))),
    (3, ((1, 2, 0), (-1, 2, 0))),
)
TREE4 = (
    (0, LEAVES), (0, ((-1, 8, 4),)), (1, ((1, 6, 4), (-1, 6, 4), (1, 2, 0), (-1, 2, 0))), (2, ((1, 4, 0), (-1, 4, 0))),
)
TREES = (TREE2, TREE2, TREE4, TREE4)
ORDER = (
    ("m", 0), ("z", 0, 0), ("f", 2), ("k", 0), ("m", 1), ("z", 1, 0), ("z", 0, 1), ("f", 3), ("z", 0, 2), ("k", 0),
    ("z", 1, 1), ("m", 2), ("z", 2, 0), ("m", 3), ("z", 3, 0), ("k", 0), ("z", 0, 3), ("z", 2, 1), ("z", 1, 2),
    ("z", 3, 1), ("e", 0), ("z", 2, 2), ("z", 1, 3), ("z", 3, 2), ("e", 1), ("e", 2), ("e", 3),
)
COUNTS = (("c", 1, 1, 0), ("x", 1, 2, 1), ("z", 1, 1, 0), ("z", 2, 4, 3))
COUNT_MSGS = sum(up + down for _, _, up, down in COUNTS)
SENDS, RECVS = 21, 59


def kernel(
    nz, slots, tok,
    gate_hbm, lift_hbm, cot_hbm, arrival_hbm, owner_hbm, mult_hbm, pieces_hbm,
    out,
    gate, lift, cot, arrival, owner, mult, pieces, in_sem,
    W, B, C, CT, H, HS, PR, ZS, ZR, CS, CR, R, out_sem,
    ssem, rsem,
):
    T = slots * tok
    nq = len(WIDTHS)
    half = sum(WIDTHS)
    offs = [sum(WIDTHS[:q]) for q in range(nq)]
    part = T // NY
    low, high = pl.ds(0, NX // 2), pl.ds(NX // 2, NX // 2)

    dp = lax.axis_index("dp")
    y = lax.axis_index("mp")
    x = dp // (NC * nz)
    z = (dp // NC) % nz
    c = dp % NC
    turn = 1 - 2 * c

    def dev(dx=0, dy=0, dz=0, flip=False):
        xx = (x + dx + NX) % NX
        yy = (y + dy + NY) % NY
        zz = (z + dz + nz) % nz
        cc = 1 - c if flip else c
        return (xx * (NC * nz) + zz * NC + cc, yy)

    sids, rids = iter(range(SENDS)), iter(range(RECVS))
    every = []

    def copy(src, dst, to, i, j):
        return pltpu.make_async_remote_copy(
            src_ref=src, dst_ref=dst, send_sem=ssem.at[i], recv_sem=rsem.at[j],
            device_id=to, device_id_type=MESH,
        )

    def send(src, dst, to, i=None, j=None):
        if i is None:
            i = next(sids)
            own = True
        else:
            own = False
        d = copy(src, dst, to, i, next(rids) if j is None else j)
        d.start()
        if own:
            every.append(d)
        return d

    s_count, s_b, s_c, s_quarter, s_core = (next(sids) for _ in range(5))
    s_h = [next(sids) for _ in range(nq)]
    s_z = [next(sids) for _ in range(nq)]
    r_b, r_c, r_core = (next(rids) for _ in range(3))
    r_h = [next(rids) for _ in range(nq)]

    loads = [
        pltpu.make_async_copy(cot_hbm, cot, in_sem.at[0]),
        pltpu.make_async_copy(gate_hbm, gate, in_sem.at[1]),
        pltpu.make_async_copy(lift_hbm, lift, in_sem.at[2]),
        pltpu.make_async_copy(arrival_hbm, arrival, in_sem.at[3]),
        pltpu.make_async_copy(owner_hbm, owner, in_sem.at[4]),
        pltpu.make_async_copy(mult_hbm, mult, in_sem.at[5]),
        pltpu.make_async_copy(pieces_hbm, pieces, in_sem.at[6]),
    ]
    for d in loads:
        d.start()

    near = [dev(flip=True)] + [dev(dx=d) for d in (1, 2, 3)] + [dev(dy=d) for d in (1, 2, 3)]
    for h in (1, 2):
        near += [dev(dz=h), dev(dz=-h)]
    barrier = pltpu.get_barrier_semaphore()
    for n in near:
        pl.semaphore_signal(barrier, inc=1, device_id=n, device_id_type=MESH)
    pl.semaphore_wait(barrier, len(near))

    for d in loads[3:]:
        d.wait()
    tiles = [pieces[owner[0, k]] for k in range(slots)]
    weights = [arrival[0] * mult[0, k] for k in range(slots)]
    count = sum(w * t for w, t in zip(weights, tiles)).astype(jnp.float32)

    loads[0].wait()
    token = lax.broadcasted_iota(jnp.int32, (part, 1), 0)
    for t in range(NY):
        scale = jnp.zeros((part, 1), jnp.float32)
        for k in range(slots):
            here = (token + t * part >= k * tok) & (token + t * part < (k + 1) * tok)
            scale = jnp.where(here, weights[k].astype(jnp.float32), scale)
        W[t] = (cot[pl.ds(t * part, part), :].astype(jnp.float32) * scale).astype(jnp.bfloat16)
    for d in (2, 1, 3):
        send(W.at[(y + d) % NY], B.at[NY - d], dev(dy=d), s_b, r_b)
    B[0] = W[y]

    def count_rounds():
        total = jnp.full((8, 128), count, jnp.float32)
        slot = 0
        for kind, hop, up, down in COUNTS:
            last = [total, total]
            got = [None, None]
            for step in range(max(up, down) + 1):
                for side, (sign, n) in enumerate(((1, up), (-1, down))):
                    if 0 < step <= n:
                        d, at = got[side]
                        d.wait_recv()
                        last[side] = CR[at] + (total if step < n else 0.0)
                    if step < n:
                        CS[slot] = last[side]
                        to = {"c": dev(flip=True), "x": dev(dx=sign * hop), "z": dev(dz=sign * hop)}[kind]
                        got[side] = (send(CS.at[slot], CR.at[slot], to, s_count), slot)
                        slot += 1
                if step < max(up, down):
                    yield
            total = total + last[0]
            if down:
                total = total + last[1]
        CS[slot] = total

    rounds = count_rounds()

    def count_step():
        next(rounds, None)

    count_step()
    loads[1].wait()
    loads[2].wait()

    def hidden(k, which, q):
        rows = pl.ds(k * tok, tok)
        cols = pl.ds(pl.multiple_of(which * half + offs[q], 128), WIDTHS[q])
        g = gate[rows, cols].astype(jnp.float32)
        u = lift[rows, cols].astype(jnp.float32)
        h = g / (1.0 + jnp.exp(-g)) * u
        row = lax.broadcasted_iota(jnp.int32, h.shape, 0)
        return jnp.where(row < tiles[k] * TILE, h, 0.0).astype(jnp.bfloat16)

    h_core, h_up, h_dn = {}, {}, {}

    def x_send(q, k):
        if k == 1:
            h_core[q].wait_recv()
        h_up[q, k] = send(H[q].at[0, k], H[q].at[3, k], dev(dx=1), s_h[q], r_h[q] if k == 0 else None)
        h_dn[q, k] = send(H[q].at[0, k], H[q].at[1, k], dev(dx=-1), s_h[q], r_h[q] if k == 1 else None)

    def forward(q):
        h_dn[q, 0].wait_recv()
        send(H[q].at[1, 0], H[q].at[2, 0], dev(dx=-1), s_h[q], r_h[q])
        h_up[q, 1].wait_recv()
        send(H[q].at[3, 1], H[q].at[2, 1], dev(dx=1), s_h[q], r_h[q])

    for q in range(nq):
        for k in range(slots):
            HS[q][pl.ds(k * tok, tok), :] = hidden(k, 1 - c, q)
        h_core[q] = send(HS[q], H[q].at[0, 1], dev(flip=True))
        for k in range(slots):
            H[q][0, 0, pl.ds(k * tok, tok), :] = hidden(k, c, q)
        if q == 0:
            x_send(0, 0)
            x_send(0, 1)

    copy(B.at[pl.ds(1, 3)], B.at[pl.ds(1, 3)], dev(dy=1), s_b, r_b).wait_recv()
    for d in (2, 1, 3):
        send(B.at[(x + d + NY - y) % NY], C.at[0, y, NX - d], dev(dx=d), s_c, r_c)
    C[0, y, 0] = B[(x + NY - y) % NY]
    count_step()
    forward(0)
    x_send(1, 0)
    x_send(1, 1)
    copy(B.at[pl.ds(1, 3)], C.at[0, y, pl.ds(1, 3)], dev(dx=1), s_c, r_c).wait_recv()
    count_step()

    def pair(rs, sign):
        i, j = s_quarter, next(rids)
        to = dev(dy=sign)
        out = copy(C.at[0, y, rs], C.at[0, y, rs], to, i, j)
        out.start()
        t = (y - sign + NY) % NY
        return copy(C.at[0, t, rs], C.at[0, t, rs], to, i, j)

    q_u1 = pair(high, 1)
    q_d1 = pair(low, -1)
    q_u2 = pair(low, 1)
    q_d2 = pair(high, -1)
    before, after, across = (y + NY - 1) % NY, (y + 1) % NY, (y + 2) % NY

    def to_core(t):
        send(C.at[0, t], C.at[1, t], dev(flip=True), s_core, r_core)

    to_core(y)
    x_send(2, 0)
    x_send(2, 1)
    q_u1.wait_recv()
    i, j = s_quarter, next(rids)
    out_u = copy(C.at[0, before, high], C.at[0, before, high], dev(dy=1), i, j)
    in_u = copy(C.at[0, across, high], C.at[0, across, high], dev(dy=1), i, j)
    out_u.start()
    q_d1.wait_recv()
    i, j = s_quarter, next(rids)
    out_d = copy(C.at[0, after, low], C.at[0, after, low], dev(dy=-1), i, j)
    in_d = copy(C.at[0, across, low], C.at[0, across, low], dev(dy=-1), i, j)
    out_d.start()
    count_step()
    forward(1)
    x_send(3, 0)
    x_send(3, 1)
    q_u2.wait_recv()
    to_core(before)
    q_d2.wait_recv()
    to_core(after)
    count_step()
    in_u.wait_recv()
    in_d.wait_recv()
    to_core(across)
    copy(C.at[0], C.at[1], dev(flip=True), s_core, r_core).wait_recv()
    pieces_ = [C[k, t, r] for r in range(NX) for k in range(NC) for t in range(NY)]
    CT[...] = jnp.concatenate(pieces_, axis=0).T

    zsem = {(q, g): (s_z[q], next(rids)) for q in range(nq) for g in range(len(TREES[q]))}
    first = {}
    for q in range(nq):
        n = 0
        for g, (_, group) in enumerate(TREES[q]):
            first[q, g] = n
            n += len(group)
    waited = set()

    def z_group(q, g):
        at = pl.ds(first[q, g], len(TREES[q][g][1]))
        return copy(ZS[q].at[at], ZR[q].at[at], dev(dz=1), *zsem[q, g])

    def z_sum(q, sign, dist):
        v = PR[q][(z + turn * sign * dist + nz) % nz]
        for g, (_, group) in enumerate(TREES[q]):
            for i, (way, _, to) in enumerate(group):
                if to == dist and (way == sign or dist == 0):
                    if (q, g) not in waited:
                        waited.add((q, g))
                        z_group(q, g).wait_recv()
                    v = v + ZR[q][first[q, g] + i].astype(jnp.float32)
        return v

    def product(q):
        four = H[q].at[pl.ds(2, 2)]
        copy(four, four, dev(dx=1), s_h[q], r_h[q]).wait_recv()
        rhs = H[q][...].reshape(NX * NC * T, WIDTHS[q])
        for m in range(4):
            acc = jnp.dot(CT[pl.ds(m * 128, 128), :], rhs, preferred_element_type=jnp.float32)
            PR[q][pl.ds(m * (nz // 4), nz // 4)] = acc.reshape(nz // 4, 128 * 4 // nz, WIDTHS[q])

    def z_step(q, s):
        for g, (step, group) in enumerate(TREES[q]):
            if step == s:
                for i, (sign, dist, to) in enumerate(group):
                    slot = first[q, g] + i
                    ZS[q][slot] = z_sum(q, sign, dist).astype(jnp.bfloat16)
                    copy(ZS[q].at[slot], ZR[q].at[slot], dev(dz=turn * sign * (dist - to)), *zsem[q, g]).start()

    fin = []

    def end(q):
        for _ in rounds:
            pass
        total = CS[COUNT_MSGS][0:1, 0:1] * float(TILE)
        R[q][...] = (z_sum(q, 1, 0) / total).reshape(R[q].shape)
        cols = out.at[:, pl.ds(pl.multiple_of(c * half + offs[q], 128), WIDTHS[q])]
        theirs = out.at[:, pl.ds(pl.multiple_of((1 - c) * half + offs[q], 128), WIDTHS[q])]
        i, j = next(sids), next(rids)
        d = copy(R[q].at[1 - c], cols, dev(flip=True), i, j)
        d.start()
        every.append(d)
        fin.append(copy(R[q].at[1 - c], theirs, dev(flip=True), i, j).wait_recv)
        d = pltpu.make_async_copy(R[q].at[c], cols, out_sem.at[q])
        d.start()
        fin.append(d.wait)

    for event in ORDER:
        q = event[1]
        if event[0] == "s":
            x_send(q, 0)
            x_send(q, 1)
        elif event[0] == "k":
            count_step()
        elif event[0] == "f":
            forward(q)
        elif event[0] == "m":
            product(q)
        elif event[0] == "z":
            z_step(q, event[2])
        else:
            end(q)
    for wait in fin:
        wait()
    for d in every:
        d.wait_send()
    groups = [(s_count, CS.at[pl.ds(0, COUNT_MSGS)]), (s_b, B.at[pl.ds(0, 3)]), (s_c, B.at[pl.ds(0, 3)])]
    groups += [(s_quarter, C.at[0, pl.ds(0, 3)]), (s_core, C.at[0])]
    for q in range(nq):
        groups += [(s_h[q], H[q].at[pl.ds(0, 3)]), (s_z[q], ZS[q])]
    for i, ref in groups:
        copy(ref, ref, dev(dx=1), i, r_b).wait_send()


def on_device(nz, gate, lift, cot, arrival, owner, mult, pieces):
    _, slots, tok, ff = gate.shape
    db = cot.shape[3]
    T = slots * tok
    rows = db // nz
    bf, f32 = jnp.bfloat16, jnp.float32
    V = pltpu.VMEM
    any_ = pl.BlockSpec(memory_space=pl.ANY)
    zbuf = [V((sum(len(g) for _, g in tree), rows, w), bf) for tree, w in zip(TREES, WIDTHS)]
    n = COUNT_MSGS
    return pl.pallas_call(
        functools.partial(kernel, nz, slots, tok),
        out_shape=jax.ShapeDtypeStruct((rows // NC, ff), f32),
        in_specs=[any_] * 7,
        out_specs=any_,
        scratch_shapes=[
            V((T, ff), bf), V((T, ff), bf), V((T, db), bf),
            *(pltpu.SMEM(a.shape, jnp.int32) for a in (arrival, owner, mult, pieces)), pltpu.SemaphoreType.DMA((7,)),
            V((NY, T // NY, db), bf), V((NY, T // NY, db), bf),
            V((NC, NY, NX, T // NY, db), bf), V((db, NX * NC * T), bf),
            [V((NX, NC, T, w), bf) for w in WIDTHS],
            [V((T, w), bf) for w in WIDTHS],
            [V((nz, rows, w), f32) for w in WIDTHS],
            zbuf, list(zbuf),
            V((n + 1, 8, 128), f32), V((n, 8, 128), f32),
            [V((NC, rows // NC, w), f32) for w in WIDTHS],
            pltpu.SemaphoreType.DMA((len(WIDTHS),)),
            pltpu.SemaphoreType.DMA((SENDS,)), pltpu.SemaphoreType.DMA((RECVS,)),
        ],
        compiler_params=pltpu.CompilerParams(
            collective_id=0, has_side_effects=True, vmem_limit_bytes=60 * 1024 * 1024
        ),
    )(
        gate.reshape(T, ff), lift.reshape(T, ff), cot.reshape(T, db),
        arrival, owner, mult, pieces,
    )


def solution(mesh):
    nz = mesh.shape["dp"] // (NX * NC)
    return jax.shard_map(
        functools.partial(on_device, nz),
        mesh=mesh,
        in_specs=(
            P("dp", None, None, "mp"),
            P("dp", None, None, "mp"),
            P("dp", None, None, "mp"),
            P("dp"),
            P("dp", None),
            P("dp", None),
            P(),
        ),
        out_specs=P("dp", "mp"),
        check_vma=False,
    )
```

```python
import functools

import jax
import jax.numpy as jnp
from jax import lax
from jax.experimental import pallas as pl
from jax.experimental.pallas import tpu as pltpu
from jax.sharding import PartitionSpec as P

MESH = pl.DeviceIdType.MESH
TILE = 32
NX = 4
NY = 4
NC = 2
WIDTHS = (256, 256, 256, 128)
BOTH = (1, -1)
LEAVES = tuple((g, d, d - 1) for d in (7, 5, 3, 1) for g in BOTH)
TREE2 = (
    (0, LEAVES), (0, ((-1, 8, 6),)), (1, ((1, 6, 4), (-1, 6, 4))), (2, ((1, 4, 2), (-1, 4, 2))),
    (3, ((1, 2, 0), (-1, 2, 0))),
)
TREE4 = (
    (0, LEAVES), (0, ((-1, 8, 4),)), (1, ((1, 6, 4), (-1, 6, 4), (1, 2, 0), (-1, 2, 0))), (2, ((1, 4, 0), (-1, 4, 0))),
)
TREES = (TREE2, TREE2, TREE4, TREE4)
ORDER = (
    ("m", 0), ("z", 0, 0), ("f", 2), ("k", 0), ("m", 1), ("z", 1, 0), ("f", 3), ("z", 0, 1), ("k", 0),
    ("m", 2), ("z", 2, 0), ("z", 1, 1), ("z", 0, 2), ("m", 3), ("z", 3, 0), ("z", 2, 1), ("z", 1, 2), ("z", 3, 1),
    ("z", 2, 2), ("k", 0), ("z", 0, 3), ("z", 3, 2), ("z", 1, 3), ("e", 0), ("e", 1), ("e", 2), ("e", 3),
)
COUNTS = (("c", 1, 1, 0), ("x", 1, 2, 1), ("z", 1, 1, 0), ("z", 2, 4, 3))
COUNT_MSGS = sum(up + down for _, _, up, down in COUNTS)
SENDS, RECVS = 21, 59


def kernel(
    nz, slots, tok,
    gate_hbm, lift_hbm, cot_hbm, arrival_hbm, owner_hbm, mult_hbm, pieces_hbm,
    out,
    gate, lift, cot, arrival, owner, mult, pieces, in_sem,
    W, B, C, CT, H, HS, PR, ZS, ZR, CS, CR, R, out_sem,
    ssem, rsem,
):
    T = slots * tok
    nq = len(WIDTHS)
    half = sum(WIDTHS)
    offs = [sum(WIDTHS[:q]) for q in range(nq)]
    part = T // NY
    low, high = pl.ds(0, NX // 2), pl.ds(NX // 2, NX // 2)

    dp = lax.axis_index("dp")
    y = lax.axis_index("mp")
    x = dp // (NC * nz)
    z = (dp // NC) % nz
    c = dp % NC
    turn = 1 - 2 * c

    def dev(dx=0, dy=0, dz=0, flip=False):
        xx = (x + dx + NX) % NX
        yy = (y + dy + NY) % NY
        zz = (z + dz + nz) % nz
        cc = 1 - c if flip else c
        return (xx * (NC * nz) + zz * NC + cc, yy)

    sids, rids = iter(range(SENDS)), iter(range(RECVS))
    every = []

    def copy(src, dst, to, i, j):
        return pltpu.make_async_remote_copy(
            src_ref=src, dst_ref=dst, send_sem=ssem.at[i], recv_sem=rsem.at[j],
            device_id=to, device_id_type=MESH,
        )

    def send(src, dst, to, i=None, j=None):
        if i is None:
            i = next(sids)
            own = True
        else:
            own = False
        d = copy(src, dst, to, i, next(rids) if j is None else j)
        d.start()
        if own:
            every.append(d)
        return d

    s_count, s_b, s_c, s_quarter, s_core = (next(sids) for _ in range(5))
    s_h = [next(sids) for _ in range(nq)]
    s_z = [next(sids) for _ in range(nq)]
    r_b, r_c, r_core = (next(rids) for _ in range(3))
    r_h = [next(rids) for _ in range(nq)]

    loads = [
        pltpu.make_async_copy(cot_hbm, cot, in_sem.at[0]),
        pltpu.make_async_copy(gate_hbm, gate, in_sem.at[1]),
        pltpu.make_async_copy(lift_hbm, lift, in_sem.at[2]),
        pltpu.make_async_copy(arrival_hbm, arrival, in_sem.at[3]),
        pltpu.make_async_copy(owner_hbm, owner, in_sem.at[4]),
        pltpu.make_async_copy(mult_hbm, mult, in_sem.at[5]),
        pltpu.make_async_copy(pieces_hbm, pieces, in_sem.at[6]),
    ]
    for d in loads:
        d.start()

    near = [dev(flip=True)] + [dev(dx=d) for d in (1, 2, 3)] + [dev(dy=d) for d in (1, 2, 3)]
    for h in (1, 2):
        near += [dev(dz=h), dev(dz=-h)]
    barrier = pltpu.get_barrier_semaphore()
    for n in near:
        pl.semaphore_signal(barrier, inc=1, device_id=n, device_id_type=MESH)
    pl.semaphore_wait(barrier, len(near))

    for d in loads[3:]:
        d.wait()
    tiles = [pieces[owner[0, k]] for k in range(slots)]
    weights = [arrival[0] * mult[0, k] for k in range(slots)]
    count = sum(w * t for w, t in zip(weights, tiles)).astype(jnp.float32)

    loads[0].wait()
    token = lax.broadcasted_iota(jnp.int32, (part, 1), 0)
    for t in range(NY):
        scale = jnp.zeros((part, 1), jnp.float32)
        for k in range(slots):
            here = (token + t * part >= k * tok) & (token + t * part < (k + 1) * tok)
            scale = jnp.where(here, weights[k].astype(jnp.float32), scale)
        W[t] = (cot[pl.ds(t * part, part), :].astype(jnp.float32) * scale).astype(jnp.bfloat16)
    for d in (2, 1, 3):
        send(W.at[(y + d) % NY], B.at[NY - d], dev(dy=d), s_b, r_b)
    B[0] = W[y]

    def count_rounds():
        total = jnp.full((8, 128), count, jnp.float32)
        slot = 0
        for kind, hop, up, down in COUNTS:
            last = [total, total]
            got = [None, None]
            for step in range(max(up, down) + 1):
                for side, (sign, n) in enumerate(((1, up), (-1, down))):
                    if 0 < step <= n:
                        d, at = got[side]
                        d.wait_recv()
                        last[side] = CR[at] + (total if step < n else 0.0)
                    if step < n:
                        CS[slot] = last[side]
                        to = {"c": dev(flip=True), "x": dev(dx=sign * hop), "z": dev(dz=sign * hop)}[kind]
                        got[side] = (send(CS.at[slot], CR.at[slot], to, s_count), slot)
                        slot += 1
                if step < max(up, down):
                    yield
            total = total + last[0]
            if down:
                total = total + last[1]
        CS[slot] = total

    rounds = count_rounds()

    def count_step():
        next(rounds, None)

    count_step()
    loads[1].wait()
    loads[2].wait()

    def hidden(k, which, q):
        rows = pl.ds(k * tok, tok)
        cols = pl.ds(pl.multiple_of(which * half + offs[q], 128), WIDTHS[q])
        g = gate[rows, cols].astype(jnp.float32)
        u = lift[rows, cols].astype(jnp.float32)
        h = g / (1.0 + jnp.exp(-g)) * u
        row = lax.broadcasted_iota(jnp.int32, h.shape, 0)
        return jnp.where(row < tiles[k] * TILE, h, 0.0).astype(jnp.bfloat16)

    h_core, h_up, h_dn = {}, {}, {}

    def x_send(q, k):
        if k == 1:
            h_core[q].wait_recv()
        h_up[q, k] = send(H[q].at[0, k], H[q].at[3, k], dev(dx=1), s_h[q], r_h[q] if k == 0 else None)
        h_dn[q, k] = send(H[q].at[0, k], H[q].at[1, k], dev(dx=-1), s_h[q], r_h[q] if k == 1 else None)

    def forward(q):
        h_dn[q, 0].wait_recv()
        send(H[q].at[1, 0], H[q].at[2, 0], dev(dx=-1), s_h[q], r_h[q])
        h_up[q, 1].wait_recv()
        send(H[q].at[3, 1], H[q].at[2, 1], dev(dx=1), s_h[q], r_h[q])

    for q in range(nq):
        for k in range(slots):
            HS[q][pl.ds(k * tok, tok), :] = hidden(k, 1 - c, q)
        h_core[q] = send(HS[q], H[q].at[0, 1], dev(flip=True))
        for k in range(slots):
            H[q][0, 0, pl.ds(k * tok, tok), :] = hidden(k, c, q)
        if q == 0:
            x_send(0, 0)
            x_send(0, 1)

    copy(B.at[pl.ds(1, 3)], B.at[pl.ds(1, 3)], dev(dy=1), s_b, r_b).wait_recv()
    for d in (2, 1, 3):
        send(B.at[(x + d + NY - y) % NY], C.at[0, y, NX - d], dev(dx=d), s_c, r_c)
    C[0, y, 0] = B[(x + NY - y) % NY]
    count_step()
    forward(0)
    x_send(1, 0)
    x_send(1, 1)
    copy(B.at[pl.ds(1, 3)], C.at[0, y, pl.ds(1, 3)], dev(dx=1), s_c, r_c).wait_recv()
    count_step()

    def pair(rs, sign):
        i, j = s_quarter, next(rids)
        to = dev(dy=sign)
        out = copy(C.at[0, y, rs], C.at[0, y, rs], to, i, j)
        out.start()
        t = (y - sign + NY) % NY
        return copy(C.at[0, t, rs], C.at[0, t, rs], to, i, j)

    q_u1 = pair(high, 1)
    q_d1 = pair(low, -1)
    q_u2 = pair(low, 1)
    q_d2 = pair(high, -1)
    before, after, across = (y + NY - 1) % NY, (y + 1) % NY, (y + 2) % NY

    def to_core(t):
        send(C.at[0, t], C.at[1, t], dev(flip=True), s_core, r_core)

    to_core(y)
    x_send(2, 0)
    x_send(2, 1)
    q_u1.wait_recv()
    i, j = s_quarter, next(rids)
    out_u = copy(C.at[0, before, high], C.at[0, before, high], dev(dy=1), i, j)
    in_u = copy(C.at[0, across, high], C.at[0, across, high], dev(dy=1), i, j)
    out_u.start()
    q_d1.wait_recv()
    i, j = s_quarter, next(rids)
    out_d = copy(C.at[0, after, low], C.at[0, after, low], dev(dy=-1), i, j)
    in_d = copy(C.at[0, across, low], C.at[0, across, low], dev(dy=-1), i, j)
    out_d.start()
    count_step()
    forward(1)
    x_send(3, 0)
    x_send(3, 1)
    q_u2.wait_recv()
    to_core(before)
    q_d2.wait_recv()
    to_core(after)
    count_step()
    in_u.wait_recv()
    in_d.wait_recv()
    to_core(across)
    copy(C.at[0], C.at[1], dev(flip=True), s_core, r_core).wait_recv()
    pieces_ = [C[k, t, r] for r in range(NX) for k in range(NC) for t in range(NY)]
    CT[...] = jnp.concatenate(pieces_, axis=0).T

    zsem = {(q, g): (s_z[q], next(rids)) for q in range(nq) for g in range(len(TREES[q]))}
    first = {}
    for q in range(nq):
        n = 0
        for g, (_, group) in enumerate(TREES[q]):
            first[q, g] = n
            n += len(group)
    waited = set()

    def z_group(q, g):
        at = pl.ds(first[q, g], len(TREES[q][g][1]))
        return copy(ZS[q].at[at], ZR[q].at[at], dev(dz=1), *zsem[q, g])

    def z_sum(q, sign, dist):
        v = PR[q][(z + turn * sign * dist + nz) % nz]
        for g, (_, group) in enumerate(TREES[q]):
            for i, (way, _, to) in enumerate(group):
                if to == dist and (way == sign or dist == 0):
                    if (q, g) not in waited:
                        waited.add((q, g))
                        z_group(q, g).wait_recv()
                    v = v + ZR[q][first[q, g] + i].astype(jnp.float32)
        return v

    def product(q):
        four = H[q].at[pl.ds(2, 2)]
        copy(four, four, dev(dx=1), s_h[q], r_h[q]).wait_recv()
        rhs = H[q][...].reshape(NX * NC * T, WIDTHS[q])
        for m in range(4):
            acc = jnp.dot(CT[pl.ds(m * 128, 128), :], rhs, preferred_element_type=jnp.float32)
            PR[q][pl.ds(m * (nz // 4), nz // 4)] = acc.reshape(nz // 4, 128 * 4 // nz, WIDTHS[q])

    def z_step(q, s):
        for g, (step, group) in enumerate(TREES[q]):
            if step == s:
                for i, (sign, dist, to) in enumerate(group):
                    slot = first[q, g] + i
                    ZS[q][slot] = z_sum(q, sign, dist).astype(jnp.bfloat16)
                    copy(ZS[q].at[slot], ZR[q].at[slot], dev(dz=turn * sign * (dist - to)), *zsem[q, g]).start()

    fin = []

    def end(q):
        for _ in rounds:
            pass
        total = CS[COUNT_MSGS][0:1, 0:1] * float(TILE)
        R[q][...] = (z_sum(q, 1, 0) / total).reshape(R[q].shape)
        cols = out.at[:, pl.ds(pl.multiple_of(c * half + offs[q], 128), WIDTHS[q])]
        theirs = out.at[:, pl.ds(pl.multiple_of((1 - c) * half + offs[q], 128), WIDTHS[q])]
        i, j = next(sids), next(rids)
        d = copy(R[q].at[1 - c], cols, dev(flip=True), i, j)
        d.start()
        every.append(d)
        fin.append(copy(R[q].at[1 - c], theirs, dev(flip=True), i, j).wait_recv)
        d = pltpu.make_async_copy(R[q].at[c], cols, out_sem.at[q])
        d.start()
        fin.append(d.wait)

    for event in ORDER:
        q = event[1]
        if event[0] == "s":
            x_send(q, 0)
            x_send(q, 1)
        elif event[0] == "k":
            count_step()
        elif event[0] == "f":
            forward(q)
        elif event[0] == "m":
            product(q)
        elif event[0] == "z":
            z_step(q, event[2])
        else:
            end(q)
    for wait in fin:
        wait()
    for d in every:
        d.wait_send()
    groups = [(s_count, CS.at[pl.ds(0, COUNT_MSGS)]), (s_b, B.at[pl.ds(0, 3)]), (s_c, B.at[pl.ds(0, 3)])]
    groups += [(s_quarter, C.at[0, pl.ds(0, 3)]), (s_core, C.at[0])]
    for q in range(nq):
        groups += [(s_h[q], H[q].at[pl.ds(0, 3)]), (s_z[q], ZS[q])]
    for i, ref in groups:
        copy(ref, ref, dev(dx=1), i, r_b).wait_send()


def on_device(nz, gate, lift, cot, arrival, owner, mult, pieces):
    _, slots, tok, ff = gate.shape
    db = cot.shape[3]
    T = slots * tok
    rows = db // nz
    bf, f32 = jnp.bfloat16, jnp.float32
    V = pltpu.VMEM
    any_ = pl.BlockSpec(memory_space=pl.ANY)
    zbuf = [V((sum(len(g) for _, g in tree), rows, w), bf) for tree, w in zip(TREES, WIDTHS)]
    n = COUNT_MSGS
    return pl.pallas_call(
        functools.partial(kernel, nz, slots, tok),
        out_shape=jax.ShapeDtypeStruct((rows // NC, ff), f32),
        in_specs=[any_] * 7,
        out_specs=any_,
        scratch_shapes=[
            V((T, ff), bf), V((T, ff), bf), V((T, db), bf),
            *(pltpu.SMEM(a.shape, jnp.int32) for a in (arrival, owner, mult, pieces)), pltpu.SemaphoreType.DMA((7,)),
            V((NY, T // NY, db), bf), V((NY, T // NY, db), bf),
            V((NC, NY, NX, T // NY, db), bf), V((db, NX * NC * T), bf),
            [V((NX, NC, T, w), bf) for w in WIDTHS],
            [V((T, w), bf) for w in WIDTHS],
            [V((nz, rows, w), f32) for w in WIDTHS],
            zbuf, list(zbuf),
            V((n + 1, 8, 128), f32), V((n, 8, 128), f32),
            [V((NC, rows // NC, w), f32) for w in WIDTHS],
            pltpu.SemaphoreType.DMA((len(WIDTHS),)),
            pltpu.SemaphoreType.DMA((SENDS,)), pltpu.SemaphoreType.DMA((RECVS,)),
        ],
        compiler_params=pltpu.CompilerParams(
            collective_id=0, has_side_effects=True, vmem_limit_bytes=60 * 1024 * 1024
        ),
    )(
        gate.reshape(T, ff), lift.reshape(T, ff), cot.reshape(T, db),
        arrival, owner, mult, pieces,
    )


def solution(mesh):
    nz = mesh.shape["dp"] // (NX * NC)
    return jax.shard_map(
        functools.partial(on_device, nz),
        mesh=mesh,
        in_specs=(
            P("dp", None, None, "mp"),
            P("dp", None, None, "mp"),
            P("dp", None, None, "mp"),
            P("dp"),
            P("dp", None),
            P("dp", None),
            P(),
        ),
        out_specs=P("dp", "mp"),
        check_vma=False,
    )
```

```python
import functools

import jax
import jax.numpy as jnp
from jax import lax
from jax.experimental import pallas as pl
from jax.experimental.pallas import tpu as pltpu
from jax.sharding import PartitionSpec as P

MESH = pl.DeviceIdType.MESH
TILE = 32
NX = 4
NY = 4
NC = 2
WIDTHS = (256, 256, 256, 128)
BOTH = (1, -1)
LEAVES = tuple((g, d, d - 1) for d in (7, 5, 3, 1) for g in BOTH)
TREE2 = (
    (0, LEAVES), (0, ((-1, 8, 6),)), (1, ((1, 6, 4), (-1, 6, 4))), (2, ((1, 4, 2), (-1, 4, 2))),
    (3, ((1, 2, 0), (-1, 2, 0))),
)
TREE4 = (
    (0, LEAVES), (0, ((-1, 8, 4),)), (1, ((1, 6, 4), (-1, 6, 4), (1, 2, 0), (-1, 2, 0))), (2, ((1, 4, 0), (-1, 4, 0))),
)
TREES = (TREE2, TREE2, TREE4, TREE4)
ORDER = (
    ("m", 0), ("z", 0, 0), ("f", 2), ("k", 0), ("m", 1), ("z", 1, 0), ("f", 3), ("z", 0, 1), ("m", 2),
    ("z", 2, 0), ("m", 3), ("z", 3, 0), ("z", 1, 1), ("z", 2, 1), ("z", 0, 2), ("z", 3, 1), ("z", 1, 2), ("z", 2, 2),
    ("k", 0), ("z", 3, 2), ("z", 0, 3), ("k", 0), ("z", 1, 3), ("e", 0), ("e", 1), ("e", 2), ("e", 3),
)
COUNTS = (("c", 1, 1, 0), ("x", 1, 2, 1), ("z", 1, 1, 0), ("z", 2, 4, 3))
COUNT_MSGS = sum(up + down for _, _, up, down in COUNTS)
SENDS, RECVS = 21, 59


def kernel(
    nz, slots, tok,
    gate_hbm, lift_hbm, cot_hbm, arrival_hbm, owner_hbm, mult_hbm, pieces_hbm,
    out,
    gate, lift, cot, arrival, owner, mult, pieces, in_sem,
    W, B, C, CT, H, HS, PR, ZS, ZR, CS, CR, R, out_sem,
    ssem, rsem,
):
    T = slots * tok
    nq = len(WIDTHS)
    half = sum(WIDTHS)
    offs = [sum(WIDTHS[:q]) for q in range(nq)]
    part = T // NY
    low, high = pl.ds(0, NX // 2), pl.ds(NX // 2, NX // 2)

    dp = lax.axis_index("dp")
    y = lax.axis_index("mp")
    x = dp // (NC * nz)
    z = (dp // NC) % nz
    c = dp % NC
    turn = 1 - 2 * c

    def dev(dx=0, dy=0, dz=0, flip=False):
        xx = (x + dx + NX) % NX
        yy = (y + dy + NY) % NY
        zz = (z + dz + nz) % nz
        cc = 1 - c if flip else c
        return (xx * (NC * nz) + zz * NC + cc, yy)

    sids, rids = iter(range(SENDS)), iter(range(RECVS))
    every = []

    def copy(src, dst, to, i, j):
        return pltpu.make_async_remote_copy(
            src_ref=src, dst_ref=dst, send_sem=ssem.at[i], recv_sem=rsem.at[j],
            device_id=to, device_id_type=MESH,
        )

    def send(src, dst, to, i=None, j=None):
        if i is None:
            i = next(sids)
            own = True
        else:
            own = False
        d = copy(src, dst, to, i, next(rids) if j is None else j)
        d.start()
        if own:
            every.append(d)
        return d

    s_count, s_b, s_c, s_quarter, s_core = (next(sids) for _ in range(5))
    s_h = [next(sids) for _ in range(nq)]
    s_z = [next(sids) for _ in range(nq)]
    r_b, r_c, r_core = (next(rids) for _ in range(3))
    r_h = [next(rids) for _ in range(nq)]

    loads = [
        pltpu.make_async_copy(cot_hbm, cot, in_sem.at[0]),
        pltpu.make_async_copy(gate_hbm, gate, in_sem.at[1]),
        pltpu.make_async_copy(lift_hbm, lift, in_sem.at[2]),
        pltpu.make_async_copy(arrival_hbm, arrival, in_sem.at[3]),
        pltpu.make_async_copy(owner_hbm, owner, in_sem.at[4]),
        pltpu.make_async_copy(mult_hbm, mult, in_sem.at[5]),
        pltpu.make_async_copy(pieces_hbm, pieces, in_sem.at[6]),
    ]
    for d in loads:
        d.start()

    near = [dev(flip=True)] + [dev(dx=d) for d in (1, 2, 3)] + [dev(dy=d) for d in (1, 2, 3)]
    for h in (1, 2):
        near += [dev(dz=h), dev(dz=-h)]
    barrier = pltpu.get_barrier_semaphore()
    for n in near:
        pl.semaphore_signal(barrier, inc=1, device_id=n, device_id_type=MESH)
    pl.semaphore_wait(barrier, len(near))

    for d in loads[3:]:
        d.wait()
    tiles = [pieces[owner[0, k]] for k in range(slots)]
    weights = [arrival[0] * mult[0, k] for k in range(slots)]
    count = sum(w * t for w, t in zip(weights, tiles)).astype(jnp.float32)

    loads[0].wait()
    token = lax.broadcasted_iota(jnp.int32, (part, 1), 0)
    for t in range(NY):
        scale = jnp.zeros((part, 1), jnp.float32)
        for k in range(slots):
            here = (token + t * part >= k * tok) & (token + t * part < (k + 1) * tok)
            scale = jnp.where(here, weights[k].astype(jnp.float32), scale)
        W[t] = (cot[pl.ds(t * part, part), :].astype(jnp.float32) * scale).astype(jnp.bfloat16)
    for d in (2, 1, 3):
        send(W.at[(y + d) % NY], B.at[NY - d], dev(dy=d), s_b, r_b)
    B[0] = W[y]

    def count_rounds():
        total = jnp.full((8, 128), count, jnp.float32)
        slot = 0
        for kind, hop, up, down in COUNTS:
            last = [total, total]
            got = [None, None]
            for step in range(max(up, down) + 1):
                for side, (sign, n) in enumerate(((1, up), (-1, down))):
                    if 0 < step <= n:
                        d, at = got[side]
                        d.wait_recv()
                        last[side] = CR[at] + (total if step < n else 0.0)
                    if step < n:
                        CS[slot] = last[side]
                        to = {"c": dev(flip=True), "x": dev(dx=sign * hop), "z": dev(dz=sign * hop)}[kind]
                        got[side] = (send(CS.at[slot], CR.at[slot], to, s_count), slot)
                        slot += 1
                if step < max(up, down):
                    yield
            total = total + last[0]
            if down:
                total = total + last[1]
        CS[slot] = total

    rounds = count_rounds()

    def count_step():
        next(rounds, None)

    count_step()
    loads[1].wait()
    loads[2].wait()

    def hidden(k, which, q):
        rows = pl.ds(k * tok, tok)
        cols = pl.ds(pl.multiple_of(which * half + offs[q], 128), WIDTHS[q])
        g = gate[rows, cols].astype(jnp.float32)
        u = lift[rows, cols].astype(jnp.float32)
        h = g / (1.0 + jnp.exp(-g)) * u
        row = lax.broadcasted_iota(jnp.int32, h.shape, 0)
        return jnp.where(row < tiles[k] * TILE, h, 0.0).astype(jnp.bfloat16)

    h_core, h_up, h_dn = {}, {}, {}

    def x_send(q, k):
        if k == 1:
            h_core[q].wait_recv()
        h_up[q, k] = send(H[q].at[0, k], H[q].at[3, k], dev(dx=1), s_h[q], r_h[q] if k == 0 else None)
        h_dn[q, k] = send(H[q].at[0, k], H[q].at[1, k], dev(dx=-1), s_h[q], r_h[q] if k == 1 else None)

    def forward(q):
        h_dn[q, 0].wait_recv()
        send(H[q].at[1, 0], H[q].at[2, 0], dev(dx=-1), s_h[q], r_h[q])
        h_up[q, 1].wait_recv()
        send(H[q].at[3, 1], H[q].at[2, 1], dev(dx=1), s_h[q], r_h[q])

    for q in range(nq):
        for k in range(slots):
            HS[q][pl.ds(k * tok, tok), :] = hidden(k, 1 - c, q)
        h_core[q] = send(HS[q], H[q].at[0, 1], dev(flip=True))
        for k in range(slots):
            H[q][0, 0, pl.ds(k * tok, tok), :] = hidden(k, c, q)
        if q == 0:
            x_send(0, 0)
            x_send(0, 1)

    copy(B.at[pl.ds(1, 3)], B.at[pl.ds(1, 3)], dev(dy=1), s_b, r_b).wait_recv()
    for d in (2, 1, 3):
        send(B.at[(x + d + NY - y) % NY], C.at[0, y, NX - d], dev(dx=d), s_c, r_c)
    C[0, y, 0] = B[(x + NY - y) % NY]
    count_step()
    forward(0)
    x_send(1, 0)
    x_send(1, 1)
    copy(B.at[pl.ds(1, 3)], C.at[0, y, pl.ds(1, 3)], dev(dx=1), s_c, r_c).wait_recv()
    count_step()

    def pair(rs, sign):
        i, j = s_quarter, next(rids)
        to = dev(dy=sign)
        out = copy(C.at[0, y, rs], C.at[0, y, rs], to, i, j)
        out.start()
        t = (y - sign + NY) % NY
        return copy(C.at[0, t, rs], C.at[0, t, rs], to, i, j)

    q_u1 = pair(high, 1)
    q_d1 = pair(low, -1)
    q_u2 = pair(low, 1)
    q_d2 = pair(high, -1)
    before, after, across = (y + NY - 1) % NY, (y + 1) % NY, (y + 2) % NY

    def to_core(t):
        send(C.at[0, t], C.at[1, t], dev(flip=True), s_core, r_core)

    to_core(y)
    x_send(2, 0)
    x_send(2, 1)
    q_u1.wait_recv()
    i, j = s_quarter, next(rids)
    out_u = copy(C.at[0, before, high], C.at[0, before, high], dev(dy=1), i, j)
    in_u = copy(C.at[0, across, high], C.at[0, across, high], dev(dy=1), i, j)
    out_u.start()
    q_d1.wait_recv()
    i, j = s_quarter, next(rids)
    out_d = copy(C.at[0, after, low], C.at[0, after, low], dev(dy=-1), i, j)
    in_d = copy(C.at[0, across, low], C.at[0, across, low], dev(dy=-1), i, j)
    out_d.start()
    count_step()
    forward(1)
    x_send(3, 0)
    x_send(3, 1)
    q_u2.wait_recv()
    to_core(before)
    q_d2.wait_recv()
    to_core(after)
    count_step()
    in_u.wait_recv()
    in_d.wait_recv()
    to_core(across)
    copy(C.at[0], C.at[1], dev(flip=True), s_core, r_core).wait_recv()
    pieces_ = [C[k, t, r] for r in range(NX) for k in range(NC) for t in range(NY)]
    CT[...] = jnp.concatenate(pieces_, axis=0).T

    zsem = {(q, g): (s_z[q], next(rids)) for q in range(nq) for g in range(len(TREES[q]))}
    first = {}
    for q in range(nq):
        n = 0
        for g, (_, group) in enumerate(TREES[q]):
            first[q, g] = n
            n += len(group)
    waited = set()

    def z_group(q, g):
        at = pl.ds(first[q, g], len(TREES[q][g][1]))
        return copy(ZS[q].at[at], ZR[q].at[at], dev(dz=1), *zsem[q, g])

    def z_sum(q, sign, dist):
        v = PR[q][(z + turn * sign * dist + nz) % nz]
        for g, (_, group) in enumerate(TREES[q]):
            for i, (way, _, to) in enumerate(group):
                if to == dist and (way == sign or dist == 0):
                    if (q, g) not in waited:
                        waited.add((q, g))
                        z_group(q, g).wait_recv()
                    v = v + ZR[q][first[q, g] + i].astype(jnp.float32)
        return v

    def product(q):
        four = H[q].at[pl.ds(2, 2)]
        copy(four, four, dev(dx=1), s_h[q], r_h[q]).wait_recv()
        rhs = H[q][...].reshape(NX * NC * T, WIDTHS[q])
        for m in range(4):
            acc = jnp.dot(CT[pl.ds(m * 128, 128), :], rhs, preferred_element_type=jnp.float32)
            PR[q][pl.ds(m * (nz // 4), nz // 4)] = acc.reshape(nz // 4, 128 * 4 // nz, WIDTHS[q])

    def z_step(q, s):
        for g, (step, group) in enumerate(TREES[q]):
            if step == s:
                for i, (sign, dist, to) in enumerate(group):
                    slot = first[q, g] + i
                    ZS[q][slot] = z_sum(q, sign, dist).astype(jnp.bfloat16)
                    copy(ZS[q].at[slot], ZR[q].at[slot], dev(dz=turn * sign * (dist - to)), *zsem[q, g]).start()

    fin = []

    def end(q):
        for _ in rounds:
            pass
        total = CS[COUNT_MSGS][0:1, 0:1] * float(TILE)
        R[q][...] = (z_sum(q, 1, 0) / total).reshape(R[q].shape)
        cols = out.at[:, pl.ds(pl.multiple_of(c * half + offs[q], 128), WIDTHS[q])]
        theirs = out.at[:, pl.ds(pl.multiple_of((1 - c) * half + offs[q], 128), WIDTHS[q])]
        i, j = next(sids), next(rids)
        d = copy(R[q].at[1 - c], cols, dev(flip=True), i, j)
        d.start()
        every.append(d)
        fin.append(copy(R[q].at[1 - c], theirs, dev(flip=True), i, j).wait_recv)
        d = pltpu.make_async_copy(R[q].at[c], cols, out_sem.at[q])
        d.start()
        fin.append(d.wait)

    for event in ORDER:
        q = event[1]
        if event[0] == "s":
            x_send(q, 0)
            x_send(q, 1)
        elif event[0] == "k":
            count_step()
        elif event[0] == "f":
            forward(q)
        elif event[0] == "m":
            product(q)
        elif event[0] == "z":
            z_step(q, event[2])
        else:
            end(q)
    for wait in fin:
        wait()
    for d in every:
        d.wait_send()
    groups = [(s_count, CS.at[pl.ds(0, COUNT_MSGS)]), (s_b, B.at[pl.ds(0, 3)]), (s_c, B.at[pl.ds(0, 3)])]
    groups += [(s_quarter, C.at[0, pl.ds(0, 3)]), (s_core, C.at[0])]
    for q in range(nq):
        groups += [(s_h[q], H[q].at[pl.ds(0, 3)]), (s_z[q], ZS[q])]
    for i, ref in groups:
        copy(ref, ref, dev(dx=1), i, r_b).wait_send()


def on_device(nz, gate, lift, cot, arrival, owner, mult, pieces):
    _, slots, tok, ff = gate.shape
    db = cot.shape[3]
    T = slots * tok
    rows = db // nz
    bf, f32 = jnp.bfloat16, jnp.float32
    V = pltpu.VMEM
    any_ = pl.BlockSpec(memory_space=pl.ANY)
    zbuf = [V((sum(len(g) for _, g in tree), rows, w), bf) for tree, w in zip(TREES, WIDTHS)]
    n = COUNT_MSGS
    return pl.pallas_call(
        functools.partial(kernel, nz, slots, tok),
        out_shape=jax.ShapeDtypeStruct((rows // NC, ff), f32),
        in_specs=[any_] * 7,
        out_specs=any_,
        scratch_shapes=[
            V((T, ff), bf), V((T, ff), bf), V((T, db), bf),
            *(pltpu.SMEM(a.shape, jnp.int32) for a in (arrival, owner, mult, pieces)), pltpu.SemaphoreType.DMA((7,)),
            V((NY, T // NY, db), bf), V((NY, T // NY, db), bf),
            V((NC, NY, NX, T // NY, db), bf), V((db, NX * NC * T), bf),
            [V((NX, NC, T, w), bf) for w in WIDTHS],
            [V((T, w), bf) for w in WIDTHS],
            [V((nz, rows, w), f32) for w in WIDTHS],
            zbuf, list(zbuf),
            V((n + 1, 8, 128), f32), V((n, 8, 128), f32),
            [V((NC, rows // NC, w), f32) for w in WIDTHS],
            pltpu.SemaphoreType.DMA((len(WIDTHS),)),
            pltpu.SemaphoreType.DMA((SENDS,)), pltpu.SemaphoreType.DMA((RECVS,)),
        ],
        compiler_params=pltpu.CompilerParams(
            collective_id=0, has_side_effects=True, vmem_limit_bytes=60 * 1024 * 1024
        ),
    )(
        gate.reshape(T, ff), lift.reshape(T, ff), cot.reshape(T, db),
        arrival, owner, mult, pieces,
    )


def solution(mesh):
    nz = mesh.shape["dp"] // (NX * NC)
    return jax.shard_map(
        functools.partial(on_device, nz),
        mesh=mesh,
        in_specs=(
            P("dp", None, None, "mp"),
            P("dp", None, None, "mp"),
            P("dp", None, None, "mp"),
            P("dp"),
            P("dp", None),
            P("dp", None),
            P(),
        ),
        out_specs=P("dp", "mp"),
        check_vma=False,
    )
```

```python
import functools

import jax
import jax.numpy as jnp
from jax import lax
from jax.experimental import pallas as pl
from jax.experimental.pallas import tpu as pltpu
from jax.sharding import PartitionSpec as P

MESH = pl.DeviceIdType.MESH
TILE = 32
NX = 4
NY = 4
NC = 2
WIDTHS = (256, 256, 256, 128)
BOTH = (1, -1)
LEAVES = tuple((g, d, d - 1) for d in (7, 5, 3, 1) for g in BOTH)
TREE2 = (
    (0, LEAVES), (0, ((-1, 8, 6),)), (1, ((1, 6, 4), (-1, 6, 4))), (2, ((1, 4, 2), (-1, 4, 2))),
    (3, ((1, 2, 0), (-1, 2, 0))),
)
TREE4 = (
    (0, LEAVES), (0, ((-1, 8, 4),)), (1, ((1, 6, 4), (-1, 6, 4), (1, 2, 0), (-1, 2, 0))), (2, ((1, 4, 0), (-1, 4, 0))),
)
TREES = (TREE2, TREE2, TREE4, TREE4)
ORDER = (
    ("m", 0), ("z", 0, 0), ("f", 2), ("k", 0), ("m", 1), ("z", 1, 0), ("f", 3), ("z", 0, 1), ("m", 2),
    ("z", 2, 0), ("m", 3), ("z", 3, 0), ("z", 1, 1), ("z", 2, 1), ("z", 0, 2), ("z", 3, 1), ("z", 1, 2), ("z", 2, 2),
    ("k", 0), ("z", 3, 2), ("z", 0, 3), ("k", 0), ("z", 1, 3), ("e", 0), ("e", 1), ("e", 2), ("e", 3),
)
COUNTS = (("c", 1, 1, 0), ("x", 1, 2, 1), ("z", 1, 1, 0), ("z", 2, 4, 3))
COUNT_MSGS = sum(up + down for _, _, up, down in COUNTS)
SENDS, RECVS = 21, 59


def kernel(
    nz, slots, tok,
    gate_hbm, lift_hbm, cot_hbm, arrival_hbm, owner_hbm, mult_hbm, pieces_hbm,
    out,
    gate, lift, cot, arrival, owner, mult, pieces, in_sem,
    W, B, C, CT, H, HS, PR, ZS, ZR, CS, CR, R, out_sem,
    ssem, rsem,
):
    T = slots * tok
    nq = len(WIDTHS)
    half = sum(WIDTHS)
    offs = [sum(WIDTHS[:q]) for q in range(nq)]
    part = T // NY
    low, high = pl.ds(0, NX // 2), pl.ds(NX // 2, NX // 2)

    dp = lax.axis_index("dp")
    y = lax.axis_index("mp")
    x = dp // (NC * nz)
    z = (dp // NC) % nz
    c = dp % NC
    turn = 1 - 2 * c

    def dev(dx=0, dy=0, dz=0, flip=False):
        xx = (x + dx + NX) % NX
        yy = (y + dy + NY) % NY
        zz = (z + dz + nz) % nz
        cc = 1 - c if flip else c
        return (xx * (NC * nz) + zz * NC + cc, yy)

    sids, rids = iter(range(SENDS)), iter(range(RECVS))
    every = []

    def copy(src, dst, to, i, j):
        return pltpu.make_async_remote_copy(
            src_ref=src, dst_ref=dst, send_sem=ssem.at[i], recv_sem=rsem.at[j],
            device_id=to, device_id_type=MESH,
        )

    def send(src, dst, to, i=None, j=None):
        if i is None:
            i = next(sids)
            own = True
        else:
            own = False
        d = copy(src, dst, to, i, next(rids) if j is None else j)
        d.start()
        if own:
            every.append(d)
        return d

    s_count, s_b, s_c, s_quarter, s_core = (next(sids) for _ in range(5))
    s_h = [next(sids) for _ in range(nq)]
    s_z = [next(sids) for _ in range(nq)]
    r_b, r_c, r_core = (next(rids) for _ in range(3))
    r_h = [next(rids) for _ in range(nq)]

    loads = [
        pltpu.make_async_copy(cot_hbm, cot, in_sem.at[0]),
        pltpu.make_async_copy(gate_hbm, gate, in_sem.at[1]),
        pltpu.make_async_copy(lift_hbm, lift, in_sem.at[2]),
        pltpu.make_async_copy(arrival_hbm, arrival, in_sem.at[3]),
        pltpu.make_async_copy(owner_hbm, owner, in_sem.at[4]),
        pltpu.make_async_copy(mult_hbm, mult, in_sem.at[5]),
        pltpu.make_async_copy(pieces_hbm, pieces, in_sem.at[6]),
    ]
    for d in loads:
        d.start()

    near = [dev(flip=True)] + [dev(dx=d) for d in (1, 2, 3)] + [dev(dy=d) for d in (1, 2, 3)]
    for h in (1, 2):
        near += [dev(dz=h), dev(dz=-h)]
    barrier = pltpu.get_barrier_semaphore()
    for n in near:
        pl.semaphore_signal(barrier, inc=1, device_id=n, device_id_type=MESH)

    for d in loads[3:]:
        d.wait()
    tiles = [pieces[owner[0, k]] for k in range(slots)]
    weights = [arrival[0] * mult[0, k] for k in range(slots)]
    count = sum(w * t for w, t in zip(weights, tiles)).astype(jnp.float32)

    loads[0].wait()
    token = lax.broadcasted_iota(jnp.int32, (part, 1), 0)
    for t in range(NY):
        scale = jnp.zeros((part, 1), jnp.float32)
        for k in range(slots):
            here = (token + t * part >= k * tok) & (token + t * part < (k + 1) * tok)
            scale = jnp.where(here, weights[k].astype(jnp.float32), scale)
        W[t] = (cot[pl.ds(t * part, part), :].astype(jnp.float32) * scale).astype(jnp.bfloat16)
    pl.semaphore_wait(barrier, len(near))
    for d in (2, 1, 3):
        send(W.at[(y + d) % NY], B.at[NY - d], dev(dy=d), s_b, r_b)
    B[0] = W[y]

    def count_rounds():
        total = jnp.full((8, 128), count, jnp.float32)
        slot = 0
        for kind, hop, up, down in COUNTS:
            last = [total, total]
            got = [None, None]
            for step in range(max(up, down) + 1):
                for side, (sign, n) in enumerate(((1, up), (-1, down))):
                    if 0 < step <= n:
                        d, at = got[side]
                        d.wait_recv()
                        last[side] = CR[at] + (total if step < n else 0.0)
                    if step < n:
                        CS[slot] = last[side]
                        to = {"c": dev(flip=True), "x": dev(dx=sign * hop), "z": dev(dz=sign * hop)}[kind]
                        got[side] = (send(CS.at[slot], CR.at[slot], to, s_count), slot)
                        slot += 1
                if step < max(up, down):
                    yield
            total = total + last[0]
            if down:
                total = total + last[1]
        CS[slot] = total

    rounds = count_rounds()

    def count_step():
        next(rounds, None)

    count_step()
    loads[1].wait()
    loads[2].wait()

    def hidden(k, which, q):
        rows = pl.ds(k * tok, tok)
        cols = pl.ds(pl.multiple_of(which * half + offs[q], 128), WIDTHS[q])
        g = gate[rows, cols].astype(jnp.float32)
        u = lift[rows, cols].astype(jnp.float32)
        h = g / (1.0 + jnp.exp(-g)) * u
        row = lax.broadcasted_iota(jnp.int32, h.shape, 0)
        return jnp.where(row < tiles[k] * TILE, h, 0.0).astype(jnp.bfloat16)

    h_core, h_up, h_dn = {}, {}, {}

    def x_send(q, k):
        if k == 1:
            h_core[q].wait_recv()
        h_up[q, k] = send(H[q].at[0, k], H[q].at[3, k], dev(dx=1), s_h[q], r_h[q] if k == 0 else None)
        h_dn[q, k] = send(H[q].at[0, k], H[q].at[1, k], dev(dx=-1), s_h[q], r_h[q] if k == 1 else None)

    def forward(q):
        h_dn[q, 0].wait_recv()
        send(H[q].at[1, 0], H[q].at[2, 0], dev(dx=-1), s_h[q], r_h[q])
        h_up[q, 1].wait_recv()
        send(H[q].at[3, 1], H[q].at[2, 1], dev(dx=1), s_h[q], r_h[q])

    for q in range(nq):
        for k in range(slots):
            HS[q][pl.ds(k * tok, tok), :] = hidden(k, 1 - c, q)
        h_core[q] = send(HS[q], H[q].at[0, 1], dev(flip=True))
        for k in range(slots):
            H[q][0, 0, pl.ds(k * tok, tok), :] = hidden(k, c, q)
        if q == 0:
            x_send(0, 0)
            x_send(0, 1)

    copy(B.at[pl.ds(1, 3)], B.at[pl.ds(1, 3)], dev(dy=1), s_b, r_b).wait_recv()
    for d in (2, 1, 3):
        send(B.at[(x + d + NY - y) % NY], C.at[0, y, NX - d], dev(dx=d), s_c, r_c)
    C[0, y, 0] = B[(x + NY - y) % NY]
    count_step()
    forward(0)
    x_send(1, 0)
    x_send(1, 1)
    copy(B.at[pl.ds(1, 3)], C.at[0, y, pl.ds(1, 3)], dev(dx=1), s_c, r_c).wait_recv()
    count_step()

    def pair(rs, sign):
        i, j = s_quarter, next(rids)
        to = dev(dy=sign)
        out = copy(C.at[0, y, rs], C.at[0, y, rs], to, i, j)
        out.start()
        t = (y - sign + NY) % NY
        return copy(C.at[0, t, rs], C.at[0, t, rs], to, i, j)

    q_u1 = pair(high, 1)
    q_d1 = pair(low, -1)
    q_u2 = pair(low, 1)
    q_d2 = pair(high, -1)
    before, after, across = (y + NY - 1) % NY, (y + 1) % NY, (y + 2) % NY

    def to_core(t):
        send(C.at[0, t], C.at[1, t], dev(flip=True), s_core, r_core)

    to_core(y)
    x_send(2, 0)
    x_send(2, 1)
    q_u1.wait_recv()
    i, j = s_quarter, next(rids)
    out_u = copy(C.at[0, before, high], C.at[0, before, high], dev(dy=1), i, j)
    in_u = copy(C.at[0, across, high], C.at[0, across, high], dev(dy=1), i, j)
    out_u.start()
    q_d1.wait_recv()
    i, j = s_quarter, next(rids)
    out_d = copy(C.at[0, after, low], C.at[0, after, low], dev(dy=-1), i, j)
    in_d = copy(C.at[0, across, low], C.at[0, across, low], dev(dy=-1), i, j)
    out_d.start()
    count_step()
    forward(1)
    x_send(3, 0)
    x_send(3, 1)
    q_u2.wait_recv()
    to_core(before)
    q_d2.wait_recv()
    to_core(after)
    count_step()
    in_u.wait_recv()
    in_d.wait_recv()
    to_core(across)
    copy(C.at[0], C.at[1], dev(flip=True), s_core, r_core).wait_recv()
    pieces_ = [C[k, t, r] for r in range(NX) for k in range(NC) for t in range(NY)]
    CT[...] = jnp.concatenate(pieces_, axis=0).T

    zsem = {(q, g): (s_z[q], next(rids)) for q in range(nq) for g in range(len(TREES[q]))}
    first = {}
    for q in range(nq):
        n = 0
        for g, (_, group) in enumerate(TREES[q]):
            first[q, g] = n
            n += len(group)
    waited = set()

    def z_group(q, g):
        at = pl.ds(first[q, g], len(TREES[q][g][1]))
        return copy(ZS[q].at[at], ZR[q].at[at], dev(dz=1), *zsem[q, g])

    def z_sum(q, sign, dist):
        v = PR[q][(z + turn * sign * dist + nz) % nz]
        for g, (_, group) in enumerate(TREES[q]):
            for i, (way, _, to) in enumerate(group):
                if to == dist and (way == sign or dist == 0):
                    if (q, g) not in waited:
                        waited.add((q, g))
                        z_group(q, g).wait_recv()
                    v = v + ZR[q][first[q, g] + i].astype(jnp.float32)
        return v

    def product(q):
        four = H[q].at[pl.ds(2, 2)]
        copy(four, four, dev(dx=1), s_h[q], r_h[q]).wait_recv()
        rhs = H[q][...].reshape(NX * NC * T, WIDTHS[q])
        for m in range(4):
            acc = jnp.dot(CT[pl.ds(m * 128, 128), :], rhs, preferred_element_type=jnp.float32)
            PR[q][pl.ds(m * (nz // 4), nz // 4)] = acc.reshape(nz // 4, 128 * 4 // nz, WIDTHS[q])

    def z_step(q, s):
        for g, (step, group) in enumerate(TREES[q]):
            if step == s:
                for i, (sign, dist, to) in enumerate(group):
                    slot = first[q, g] + i
                    ZS[q][slot] = z_sum(q, sign, dist).astype(jnp.bfloat16)
                    copy(ZS[q].at[slot], ZR[q].at[slot], dev(dz=turn * sign * (dist - to)), *zsem[q, g]).start()

    fin = []

    def end(q):
        for _ in rounds:
            pass
        total = CS[COUNT_MSGS][0:1, 0:1] * float(TILE)
        R[q][...] = (z_sum(q, 1, 0) / total).reshape(R[q].shape)
        cols = out.at[:, pl.ds(pl.multiple_of(c * half + offs[q], 128), WIDTHS[q])]
        theirs = out.at[:, pl.ds(pl.multiple_of((1 - c) * half + offs[q], 128), WIDTHS[q])]
        i, j = next(sids), next(rids)
        d = copy(R[q].at[1 - c], cols, dev(flip=True), i, j)
        d.start()
        every.append(d)
        fin.append(copy(R[q].at[1 - c], theirs, dev(flip=True), i, j).wait_recv)
        d = pltpu.make_async_copy(R[q].at[c], cols, out_sem.at[q])
        d.start()
        fin.append(d.wait)

    for event in ORDER:
        q = event[1]
        if event[0] == "s":
            x_send(q, 0)
            x_send(q, 1)
        elif event[0] == "k":
            count_step()
        elif event[0] == "f":
            forward(q)
        elif event[0] == "m":
            product(q)
        elif event[0] == "z":
            z_step(q, event[2])
        else:
            end(q)
    for wait in fin:
        wait()
    for d in every:
        d.wait_send()
    groups = [(s_count, CS.at[pl.ds(0, COUNT_MSGS)]), (s_b, B.at[pl.ds(0, 3)]), (s_c, B.at[pl.ds(0, 3)])]
    groups += [(s_quarter, C.at[0, pl.ds(0, 3)]), (s_core, C.at[0])]
    for q in range(nq):
        groups += [(s_h[q], H[q].at[pl.ds(0, 3)]), (s_z[q], ZS[q])]
    for i, ref in groups:
        copy(ref, ref, dev(dx=1), i, r_b).wait_send()


def on_device(nz, gate, lift, cot, arrival, owner, mult, pieces):
    _, slots, tok, ff = gate.shape
    db = cot.shape[3]
    T = slots * tok
    rows = db // nz
    bf, f32 = jnp.bfloat16, jnp.float32
    V = pltpu.VMEM
    any_ = pl.BlockSpec(memory_space=pl.ANY)
    zbuf = [V((sum(len(g) for _, g in tree), rows, w), bf) for tree, w in zip(TREES, WIDTHS)]
    n = COUNT_MSGS
    return pl.pallas_call(
        functools.partial(kernel, nz, slots, tok),
        out_shape=jax.ShapeDtypeStruct((rows // NC, ff), f32),
        in_specs=[any_] * 7,
        out_specs=any_,
        scratch_shapes=[
            V((T, ff), bf), V((T, ff), bf), V((T, db), bf),
            *(pltpu.SMEM(a.shape, jnp.int32) for a in (arrival, owner, mult, pieces)), pltpu.SemaphoreType.DMA((7,)),
            V((NY, T // NY, db), bf), V((NY, T // NY, db), bf),
            V((NC, NY, NX, T // NY, db), bf), V((db, NX * NC * T), bf),
            [V((NX, NC, T, w), bf) for w in WIDTHS],
            [V((T, w), bf) for w in WIDTHS],
            [V((nz, rows, w), f32) for w in WIDTHS],
            zbuf, list(zbuf),
            V((n + 1, 8, 128), f32), V((n, 8, 128), f32),
            [V((NC, rows // NC, w), f32) for w in WIDTHS],
            pltpu.SemaphoreType.DMA((len(WIDTHS),)),
            pltpu.SemaphoreType.DMA((SENDS,)), pltpu.SemaphoreType.DMA((RECVS,)),
        ],
        compiler_params=pltpu.CompilerParams(
            collective_id=0, has_side_effects=True, vmem_limit_bytes=60 * 1024 * 1024
        ),
    )(
        gate.reshape(T, ff), lift.reshape(T, ff), cot.reshape(T, db),
        arrival, owner, mult, pieces,
    )


def solution(mesh):
    nz = mesh.shape["dp"] // (NX * NC)
    return jax.shard_map(
        functools.partial(on_device, nz),
        mesh=mesh,
        in_specs=(
            P("dp", None, None, "mp"),
            P("dp", None, None, "mp"),
            P("dp", None, None, "mp"),
            P("dp"),
            P("dp", None),
            P("dp", None),
            P(),
        ),
        out_specs=P("dp", "mp"),
        check_vma=False,
    )
```
